256 devices in a mesh: seq: 8 (over z), tensor: 8 (over x, y_hi), dp: 4 (over y_lo, core).
Axes of the slice: x: 4, y: 4 (y_hi: 2, y_lo: 2; y = y_hi * 2 + y_lo), z: 8, core: 2. Of those that a mesh axis runs over, the one named last changes fastest.
Arguments:
- tokens: bfloat16 [4, 2048, 3072], P('dp', 'seq'), may hold values from -6 to 6
- cotangent: bfloat16 [4, 2048, 3072], P('dp', 'seq'), may hold values from -6 to 6
- qkv_weight: bfloat16 [3072, 3, 3072], P(('seq', 'dp'), None, 'tensor'), may hold values from -0.109375 to 0.109375
- out_weight: bfloat16 [3072, 3072], P(('seq', 'dp'), 'tensor'), may hold values from -0.109375 to 0.109375
Outputs:
- qkv_grad: float32 [3072, 3, 3072], P(('seq', 'dp'), None, 'tensor')
- out_grad: float32 [3072, 3072], P(('seq', 'dp'), 'tensor')
- branch_grad: bfloat16 [4, 2048, 3072], P('dp', 'seq', 'tensor')
The draws below stay inside these ranges and needn't reach their ends.
All inputs are finite; a program needn't handle non-finite values.
Results may differ from the reference program's by a relative error of at most 0.025.
Values may be sent and summed in bfloat16 or wider, within the bound.
No kernel may reach another device: no remote copies, remote signals or barrier semaphores. Data moves between devices by JAX's collectives and lax.ppermute only.
A program may use at most 128 MiB of HBM per device.

```python
import jax
import jax.numpy as jnp
from jax import lax

D = 3072
HD = 128
TOK_DEV = 256
HEADS = 24
SEQ_LEN = 2048
BATCH = 4
N_SEQ = 8


def strengthened(drawn, key, source, target, blocks, factor):
    def block_of(axis_at):
        return (jnp.arange(drawn.shape[axis_at]) // (drawn.shape[axis_at] // blocks)).reshape((-1,) + (1,) * (drawn.ndim - 1 - axis_at))

    near = jax.random.permutation(key, blocks)[block_of(target)]
    second = (block_of(target) + blocks // 2) % blocks
    return jnp.where((block_of(source) == near) | (block_of(source) == second), factor * drawn, drawn)


def block_scale(stream_key, dims, shards, low, largest):
    loudness = 1.0
    for axis_at, blocks in shards:
        draws = jax.random.uniform(jax.random.fold_in(jax.random.fold_in(stream_key, 6), axis_at), (blocks,), jnp.float32, low / len(shards), largest / len(shards))
        loudness = loudness * jnp.repeat(jnp.exp(draws), dims[axis_at] // blocks).reshape((-1,) + (1,) * (len(dims) - 1 - axis_at))
    return loudness


def bell_draw(stream_key, extent, scale, most, split=(), held_as=jnp.bfloat16):
    values = jax.random.normal(stream_key, extent, jnp.float32) * scale
    if len(split) > 0:
        values = block_scale(stream_key, extent, split, -0.22, 0.18) * values
    return jnp.clip(values, min=-most, max=most).astype(held_as)


def bell_draw_with(rng, extent, scale, reach, shards, heavy, kind=jnp.bfloat16):
    result = scale * jax.random.normal(rng, extent, jnp.float32)
    if shards:
        result = result * block_scale(rng, extent, shards, -0.22, 0.18)
    return jnp.clip(strengthened(result, jax.random.fold_in(rng, 3), *heavy), -reach, reach).astype(kind)


def setup_inputs(seed: int = 0) -> dict:
    seeds = jax.random.split(jax.random.key(seed), 5)
    return {
        "tokens": bell_draw_with(seeds[0], (BATCH, SEQ_LEN, D), 1.0, 6.0, ((0, 4), (1, 8)), (1, 2, 8, 2.0)),
        "cotangent": bell_draw_with(seeds[1], (BATCH, SEQ_LEN, D), 1.0, 6.0, ((0, 4), (1, 8)), (1, 2, 8, 2.0)),
        "qkv_weight": bell_draw(seeds[2], (D, 3, HEADS * HD), D ** -0.5, 0.109375, ((0, 32), (2, 8))),
        "out_weight": bell_draw(seeds[3], (D, HEADS * HD), (HEADS * HD) ** -0.5, 0.109375, ((0, 32), (1, 8))),
    }


epsilon = 1e-06

def normalize(values):
    average = lax.optimization_barrier(jnp.mean(values, axis=-1, keepdims=True))
    centered = values - average
    inverse = lax.rsqrt(lax.optimization_barrier(jnp.mean(centered * centered, axis=-1, keepdims=True)) + epsilon)
    return (centered * inverse, inverse)

def normalize_back(gradient, normed, inverse):
    mean_grad = lax.optimization_barrier(jnp.mean(gradient, axis=-1, keepdims=True))
    mean_both = lax.optimization_barrier(jnp.mean(gradient * normed, axis=-1, keepdims=True))
    return (gradient - mean_grad - normed * mean_both) * inverse

def narrow(values):
    return lax.optimization_barrier(values.astype(jnp.bfloat16)).astype(jnp.float32)

def reference(tokens, cotangent, qkv_weight, out_weight):
    all_columns = HEADS * HD
    score_scale = HD ** (-0.5)
    flat_weight = qkv_weight.reshape(D, 3 * all_columns)
    qkv_total = jnp.zeros((D, 3 * all_columns), jnp.float32)
    out_total = jnp.zeros((D, all_columns), jnp.float32)
    branches = []
    for batch_row in range(BATCH):
        row_grads = cotangent[batch_row]
        normed, inverse = normalize(tokens[batch_row].astype(jnp.float32))
        unit_low = normed.astype(jnp.bfloat16)
        projected = jnp.dot(unit_low, flat_weight, preferred_element_type=jnp.float32)
        query_unit, query_inv = normalize(projected[:, :all_columns].reshape(SEQ_LEN, HEADS, HD))
        key_unit, key_inv = normalize(projected[:, all_columns:2 * all_columns].reshape(SEQ_LEN, HEADS, HD))
        query_low = narrow(query_unit)
        key_low = narrow(key_unit)
        value_low = narrow(projected[:, 2 * all_columns:].reshape(SEQ_LEN, HEADS, HD))
        scores = jnp.einsum('qhd,khd->hqk', query_low, key_low) * score_scale
        exponent = jnp.exp(scores)
        exp_total = lax.optimization_barrier(jnp.sum(exponent, axis=-1))
        attended = jnp.einsum('hqk,khd->qhd', narrow(exponent), value_low) / exp_total.T[:, :, None]
        attended_low = attended.astype(jnp.bfloat16)
        attended_wide = lax.optimization_barrier(attended_low).astype(jnp.float32)
        grad_low = jnp.dot(row_grads, out_weight, preferred_element_type=jnp.float32).astype(jnp.bfloat16)
        grad_wide = lax.optimization_barrier(grad_low).astype(jnp.float32).reshape(SEQ_LEN, HEADS, HD)
        row_delta = lax.optimization_barrier(jnp.sum(grad_wide * attended_wide, axis=-1))
        probability = exponent / exp_total[:, :, None]
        prob_grad = jnp.einsum('qhd,khd->hqk', grad_wide, value_low)
        grad_score = narrow(probability * (prob_grad - row_delta.T[:, :, None]) * score_scale)
        query_raw = jnp.einsum('hqk,khd->qhd', grad_score, key_low)
        key_raw = jnp.einsum('hqk,qhd->khd', grad_score, query_low)
        value_raw = jnp.einsum('hqk,qhd->khd', narrow(probability), grad_wide)
        query_back = normalize_back(query_raw, query_unit, query_inv)
        key_back = normalize_back(key_raw, key_unit, key_inv)
        qkv_low = jnp.concatenate([query_back.reshape(SEQ_LEN, all_columns), key_back.reshape(SEQ_LEN, all_columns), value_raw.reshape(SEQ_LEN, all_columns)], axis=1).astype(jnp.bfloat16)
        inner_grad = jnp.dot(qkv_low, flat_weight.T, preferred_element_type=jnp.float32)
        branches.append(normalize_back(inner_grad, normed, inverse).astype(jnp.bfloat16))
        attended_flat = attended_low.reshape(SEQ_LEN, all_columns)
        for block_index in range(N_SEQ):
            low_row = block_index * TOK_DEV
            high_row = low_row + TOK_DEV
            qkv_total = qkv_total + narrow(jnp.dot(unit_low[low_row:high_row].T, qkv_low[low_row:high_row], preferred_element_type=jnp.float32))
            out_total = out_total + narrow(jnp.dot(row_grads[low_row:high_row].T, attended_flat[low_row:high_row], preferred_element_type=jnp.float32))
    return (qkv_total.reshape(D, 3, all_columns), out_total, jnp.stack(branches))
```

```python
import jax
import jax.numpy as jnp
from jax import lax
from jax.experimental import pallas as pl
from jax.sharding import PartitionSpec as P
from jax.experimental.pallas import tpu as pltpu

HD = 128
epsilon = 1e-06
BF = jnp.bfloat16
F32 = jnp.float32
CHUNK = 256


def dot(a, b, ca=1, cb=0):
    return lax.dot_general(a, b, (((ca,), (cb,)), ((), ())), preferred_element_type=F32)


def normalize(values, axis=-1):
    average = jnp.mean(values, axis=axis, keepdims=True)
    centered = values - average
    inverse = lax.rsqrt(jnp.mean(centered * centered, axis=axis, keepdims=True) + epsilon)
    return (centered * inverse, inverse)


def normalize_back(gradient, normed, inverse, axis=-1):
    mean_grad = jnp.mean(gradient, axis=axis, keepdims=True)
    mean_both = jnp.mean(gradient * normed, axis=axis, keepdims=True)
    return (gradient - mean_grad - normed * mean_both) * inverse


def project_body(x_ref, c_ref, w_ref, q_ref, k_ref, kv_ref, g_ref, acc_ref):
    step = pl.program_id(0)
    width = g_ref.shape[1]
    rows = x_ref.shape[0]
    part = dot(x_ref[...], w_ref[:, : 3 * width])
    part_g = dot(c_ref[...], w_ref[:, 3 * width :])

    @pl.when(step == 0)
    def _():
        acc_ref[:, : 3 * width] = part
        acc_ref[:, 3 * width :] = part_g

    @pl.when(step > 0)
    def _():
        acc_ref[:, : 3 * width] += part
        acc_ref[:, 3 * width :] += part_g

    @pl.when(step == pl.num_programs(0) - 1)
    def _():
        q_ref[...] = acc_ref[:, :width]
        k_ref[...] = acc_ref[:, width : 2 * width]
        for h in range(width // HD):
            unit, _ = normalize(acc_ref[:, width + h * HD : width + (h + 1) * HD])
            kv_ref[:rows, h * HD : (h + 1) * HD] = unit.astype(BF)
        kv_ref[rows:, :] = acc_ref[:, 2 * width : 3 * width].astype(BF)
        g_ref[...] = acc_ref[:, 3 * width :].astype(BF)


def project(x, c, w, steps=8):
    rows, features = x.shape
    width = w.shape[1] // 4
    block = features // steps
    return pl.pallas_call(
        project_body,
        grid=(steps,),
        in_specs=[
            pl.BlockSpec((rows, block), lambda i: (0, i)),
            pl.BlockSpec((rows, block), lambda i: (0, i)),
            pl.BlockSpec((block, 4 * width), lambda i: (i, 0)),
        ],
        out_specs=[
            pl.BlockSpec((rows, width), lambda i: (0, 0)),
            pl.BlockSpec((rows, width), lambda i: (0, 0)),
            pl.BlockSpec((2 * rows, width), lambda i: (0, 0)),
            pl.BlockSpec((rows, width), lambda i: (0, 0)),
        ],
        out_shape=[
            jax.ShapeDtypeStruct((rows, width), F32),
            jax.ShapeDtypeStruct((rows, width), F32),
            jax.ShapeDtypeStruct((2 * rows, width), BF),
            jax.ShapeDtypeStruct((rows, width), BF),
        ],
        scratch_shapes=[pltpu.VMEM((rows, 4 * width), F32)],
        compiler_params=pltpu.CompilerParams(dimension_semantics=("arbitrary",)),
        name="project",
    )(x, c, w)


def attend_body(q_ref, g_ref, kv_ref, att_ref, qb_ref, dkv_ref, e_ref):
    blocks = kv_ref.shape[0]
    rows = q_ref.shape[0]
    keys = kv_ref.shape[2]
    scale = HD ** (-0.5)
    q_unit, q_inv = normalize(q_ref[...])
    q = q_unit.astype(BF)
    g = g_ref[...]
    total = jnp.zeros((8, rows), F32)
    att_t = jnp.zeros((HD, rows), F32)
    for j in range(blocks):
        e = jnp.exp(dot(kv_ref[j, 0], q, 1, 1) * scale)
        e_ref[j] = e
        total = total + jnp.sum(e.reshape(keys // 8, 8, rows), axis=0)
        att_t = att_t + dot(kv_ref[j, 1].T, e.astype(BF))
    total = jnp.sum(total, axis=0, keepdims=True)
    inv_total = 1.0 / total
    att = (att_t * inv_total).T.astype(BF)
    att_ref[...] = att
    delta = jnp.sum((g.astype(F32) * att.astype(F32)).T, axis=0, keepdims=True)
    dq_t = jnp.zeros((HD, rows), F32)
    for j in range(blocks):
        p = e_ref[j] * inv_total
        dp = dot(kv_ref[j, 1], g, 1, 1)
        ds = (p * ((dp - delta) * scale)).astype(BF)
        dkv_ref[j, 0] = dot(ds, q).astype(BF)
        dkv_ref[j, 1] = dot(p.astype(BF), g).astype(BF)
        dq_t = dq_t + dot(kv_ref[j, 0].T, ds)
    qb_ref[...] = normalize_back(dq_t.T, q_unit, q_inv).astype(BF)


def attend(q, g, kv):
    rows, width = q.shape
    blocks, _, keys, _ = kv.shape
    row_spec = pl.BlockSpec((rows, HD), lambda h: (0, h))
    kv_spec = pl.BlockSpec((blocks, 2, keys, HD), lambda h: (0, 0, 0, h))
    return pl.pallas_call(
        attend_body,
        grid=(width // HD,),
        in_specs=[row_spec, row_spec, kv_spec],
        out_specs=[row_spec, row_spec, kv_spec],
        out_shape=[
            jax.ShapeDtypeStruct((rows, width), BF),
            jax.ShapeDtypeStruct((rows, width), BF),
            jax.ShapeDtypeStruct(kv.shape, BF),
        ],
        scratch_shapes=[pltpu.VMEM((blocks, keys, rows), F32)],
        compiler_params=pltpu.CompilerParams(dimension_semantics=("arbitrary",)),
        name="attend",
    )(q, g, kv)


def key_back_body(s_ref, k_ref, out_ref):
    width = k_ref.shape[1]
    rows = k_ref.shape[0]
    for h in range(width // HD):
        cols = slice(h * HD, (h + 1) * HD)
        unit, inv = normalize(k_ref[:, cols])
        out_ref[:, cols] = normalize_back(s_ref[:rows, cols].astype(F32), unit, inv).astype(BF)
    out_ref[:, width:] = s_ref[rows:, :].astype(BF)


def key_back(summed, k):
    rows, width = k.shape
    return pl.pallas_call(
        key_back_body,
        out_shape=jax.ShapeDtypeStruct((rows, 2 * width), BF),
        name="key_back",
    )(summed, k)


def terms_body(me_ref, x_ref, c_ref, a_ref, b_ref, send_ref, keep_ref, *, split):
    core, ylo = me_ref[1], me_ref[2]
    own = x_ref.shape[3]
    width = a_ref.shape[1]
    for y in range(2):
        for away, out_ref in ((1, send_ref), (0, keep_ref)):
            source = (lax.rem(ylo + y, 2), lax.rem(core + away, 2))
            left = x_ref[0, source[0], source[1]]
            first = dot(left, a_ref[...])
            other = dot(c_ref[0, source[0], source[1]] if split else left, b_ref[...])
            spot = (y, 0) if split else (0, y)
            out_ref[spot[0], spot[1], :, :width] = first.astype(BF)
            out_ref[spot[0], spot[1], :, width:] = other.astype(BF)


def terms(me, x_t, c_t, a, b, split):
    slabs, _, _, own, rows = x_t.shape
    width = a.shape[1]
    slab = pl.BlockSpec((1, 2, 2, own, rows), lambda i, me: (lax.rem(me[0] + i, slabs), 0, 0, 0, 0))
    whole = pl.BlockSpec((rows, width), lambda i, me: (0, 0))
    if split:
        shape = (2, slabs, own, 2 * width)
        out = pl.BlockSpec((2, 1, own, 2 * width), lambda i, me: (0, i, 0, 0))
    else:
        shape = (slabs, 2, own, 2 * width)
        out = pl.BlockSpec((1, 2, own, 2 * width), lambda i, me: (i, 0, 0, 0))
    return pl.pallas_call(
        lambda *refs: terms_body(*refs, split=split),
        grid_spec=pltpu.PrefetchScalarGridSpec(
            num_scalar_prefetch=1,
            grid=(slabs,),
            in_specs=[slab, slab, whole, whole],
            out_specs=[out, out],
        ),
        out_shape=[jax.ShapeDtypeStruct(shape, BF)] * 2,
        compiler_params=pltpu.CompilerParams(dimension_semantics=("arbitrary",)),
        name="terms_split" if split else "terms_plain",
    )(me, x_t, c_t, a, b)


def inner_body(qb_ref, kvb_ref, w_ref, unit_ref, out_ref, sum_ref, both_ref):
    step = pl.program_id(0)
    width = qb_ref.shape[1]
    inner = dot(qb_ref[...], w_ref[:, :width], 1, 1) + dot(kvb_ref[...], w_ref[:, width:], 1, 1)
    out_ref[0] = inner.astype(BF)
    both = inner * unit_ref[...]
    lanes = range(0, inner.shape[1], HD)
    plain = sum(inner[:, i : i + HD] for i in lanes)
    times = sum(both[:, i : i + HD] for i in lanes)

    @pl.when(step == 0)
    def _():
        sum_ref[...] = plain
        both_ref[...] = times

    @pl.when(step > 0)
    def _():
        sum_ref[...] += plain
        both_ref[...] += times


def inner(qb, kvb, w, unit, shares):
    rows, width = qb.shape
    block = w.shape[0] // shares
    stat = pl.BlockSpec((rows, HD), lambda i: (0, 0))
    return pl.pallas_call(
        inner_body,
        grid=(shares,),
        in_specs=[
            pl.BlockSpec((rows, width), lambda i: (0, 0)),
            pl.BlockSpec((rows, 2 * width), lambda i: (0, 0)),
            pl.BlockSpec((block, 3 * width), lambda i: (i, 0)),
            pl.BlockSpec((rows, block), lambda i: (0, i)),
        ],
        out_specs=[pl.BlockSpec((1, rows, block), lambda i: (i, 0, 0)), stat, stat],
        out_shape=[
            jax.ShapeDtypeStruct((shares, rows, block), BF),
            jax.ShapeDtypeStruct((rows, HD), F32),
            jax.ShapeDtypeStruct((rows, HD), F32),
        ],
        compiler_params=pltpu.CompilerParams(dimension_semantics=("arbitrary",)),
        name="inner",
    )(qb, kvb, w, unit)


def swap(value, axis):
    return lax.ppermute(value, axis, [(0, 1), (1, 0)])


def plus(a, b):
    return (a.astype(F32) + b.astype(F32)).astype(BF)


def ring_reduce(parts):
    size = parts.shape[0]
    far = size // 2
    up = [(i, (i + 1) % size) for i in range(size)]
    down = [(i, (i - 1) % size) for i in range(size)]
    half = parts.shape[1] // 2
    high = lax.ppermute(parts[far, :half], "seq", up)
    low = lax.ppermute(parts[far, half:], "seq", down)
    for step in range(far - 1, 0, -1):
        if step == far - 1:
            mine, theirs = parts[step], parts[size - step]
            high = jnp.concatenate([plus(mine[:half], high), mine[half:]], axis=0)
            low = jnp.concatenate([theirs[:half], plus(theirs[half:], low)], axis=0)
        else:
            high, low = plus(parts[step], high), plus(parts[size - step], low)
        high = lax.ppermute(high, "seq", up)
        low = lax.ppermute(low, "seq", down)
    return parts[0].astype(F32) + high.astype(F32) + low.astype(F32)


def pieces_of(value):
    parts = []
    for _ in range(3):
        part = lax.reduce_precision(value, 8, 7)
        parts.append(part.astype(BF))
        value = value - part
    return parts


def local(tokens, cotangent, qkv_weight, out_weight):
    row_count, feature_count = tokens.shape[1:]
    own, _, width = qkv_weight.shape
    slabs = lax.axis_size("seq")
    shares = lax.axis_size(("x", "yhi"))
    me = jnp.stack([lax.axis_index("seq"), lax.axis_index("core"), lax.axis_index("ylo")]).astype(jnp.int32)
    grad_rows = cotangent[0]
    normed, inverse = normalize(tokens[0].astype(F32))
    unit_low = normed.astype(BF)
    x_t = unit_low.T.reshape(slabs, 2, 2, own, row_count)
    c_t = grad_rows.T.reshape(slabs, 2, 2, own, row_count)
    shard = jnp.concatenate([qkv_weight.reshape(own, 3 * width), out_weight], axis=1)
    weight = lax.all_gather(shard, ("seq", "ylo", "core"), axis=0, tiled=True)
    query, key, key_value, grad_low = project(unit_low, grad_rows, weight)
    every = lax.all_gather(key_value, "seq", axis=0, tiled=True)
    attended, query_back, pair = attend(
        query, grad_low, every.reshape(slabs, 2, row_count, width)
    )
    pair = lax.psum_scatter(
        pair.reshape(slabs * 2 * row_count, width), "seq", scatter_dimension=0, tiled=True
    )
    send, keep = terms(me, x_t, c_t, query_back, attended, True)
    half = plus(keep, swap(send, "core"))
    quarter = plus(half[0], swap(half[1], "ylo"))
    query_out = ring_reduce(quarter)
    rest_back = key_back(pair, key)
    send, keep = terms(me, x_t, x_t, rest_back[:, :width], rest_back[:, width:], False)
    share, plain, both = inner(query_back, rest_back, weight, normed, shares)
    half = plus(keep, swap(send, "core"))
    column = ring_reduce(half.reshape(slabs, 2 * own, 2 * width)).astype(BF)
    column = column.reshape(2, own, 2 * width)
    key_value_grad = column[0].astype(F32) + swap(column[1], "ylo").astype(F32)

    stats = jnp.stack(pieces_of(jnp.sum(plain, axis=1)) + pieces_of(jnp.sum(both, axis=1)))
    stats = stats.reshape(-1, share.shape[2])
    stats = jnp.pad(stats, ((0, 16 - stats.shape[0]), (0, 0)))
    load = jnp.concatenate([share, jnp.broadcast_to(stats, (shares, *stats.shape))], axis=1)
    load = lax.all_to_all(load, ("x", "yhi"), 0, 0, tiled=True).astype(F32)
    load = jnp.sum(load, axis=0)
    own_share = load[:row_count]
    totals = load[row_count:].reshape(-1)[: 6 * row_count].reshape(2, 3, row_count)
    totals = jnp.sum(totals, axis=1)[:, :, None] / feature_count
    offset = lax.axis_index(("x", "yhi")) * share.shape[2]
    unit_own = lax.dynamic_slice_in_dim(normed, offset, share.shape[2], 1)
    branch = (own_share - totals[0] - unit_own * totals[1]) * inverse
    qkv_grad = jnp.stack(
        [query_out[:, :width], key_value_grad[:, :width], key_value_grad[:, width:]], axis=1
    )
    return (qkv_grad, query_out[:, width:], branch.astype(BF)[None])


def solution(mesh):
    split = jax.sharding.Mesh(
        mesh.devices.reshape(mesh.shape["seq"], mesh.shape["tensor"] // 2, 2, 2, 2),
        ("seq", "x", "yhi", "ylo", "core"),
    )
    blocks = ("seq", "ylo", "core")
    heads = ("x", "yhi")
    return jax.shard_map(
        local,
        mesh=split,
        in_specs=(
            P(("ylo", "core"), "seq", None),
            P(("ylo", "core"), "seq", None),
            P(blocks, None, heads),
            P(blocks, heads),
        ),
        out_specs=(
            P(blocks, None, heads),
            P(blocks, heads),
            P(("ylo", "core"), "seq", heads),
        ),
        check_vma=False,
    )
```

```python
import jax
import jax.numpy as jnp
from jax import lax
from jax.experimental import pallas as pl
from jax.experimental.pallas import tpu as pltpu
from jax.sharding import PartitionSpec as P

HD = 128
epsilon = 1e-06
BF = jnp.bfloat16
F32 = jnp.float32


def dot(a, b, ca=1, cb=0):
    return lax.dot_general(a, b, (((ca,), (cb,)), ((), ())), preferred_element_type=F32)


def normalize(values, axis=-1):
    average = jnp.mean(values, axis=axis, keepdims=True)
    centered = values - average
    inverse = lax.rsqrt(jnp.mean(centered * centered, axis=axis, keepdims=True) + epsilon)
    return (centered * inverse, inverse)


def normalize_back(gradient, normed, inverse, axis=-1):
    mean_grad = jnp.mean(gradient, axis=axis, keepdims=True)
    mean_both = jnp.mean(gradient * normed, axis=axis, keepdims=True)
    return (gradient - mean_grad - normed * mean_both) * inverse


ARBITRARY = pltpu.CompilerParams(dimension_semantics=("arbitrary",))


def prepare_body(me_ref, tok_ref, cot_ref, unit_ref, inv_ref, xt_ref, xr_ref, ct_ref, cr_ref, mean_ref):
    step = pl.program_id(0)
    rows = tok_ref.shape[0]
    block = unit_ref.shape[1]
    own = block // 4

    @pl.when(step == 0)
    def _():
        values = tok_ref[...].astype(F32)
        average = jnp.mean(values, axis=-1, keepdims=True)
        centered = values - average
        inverse = lax.rsqrt(jnp.mean(centered * centered, axis=-1, keepdims=True) + epsilon)
        mean_ref[...] = jnp.broadcast_to(average, (rows, HD))
        inv_ref[...] = jnp.broadcast_to(inverse, (rows, HD))

    here = pl.ds(pl.multiple_of(step * block, HD), block)
    unit = (tok_ref[:, here].astype(F32) - mean_ref[:, :1]) * inv_ref[:, :1]
    unit_ref[...] = unit
    for value, t_ref, r_ref in (
        (unit.astype(BF), xt_ref, xr_ref),
        (cot_ref[:, here], ct_ref, cr_ref),
    ):
        turned = value.T
        for y in range(2):
            for c in range(2):
                away_y, away_c = lax.rem(me_ref[2] + y, 2), lax.rem(me_ref[1] + c, 2)
                at = (2 * y + c) * own
                t_ref[0, away_c, away_y] = turned[at : at + own]
        for c in range(2):
            r_ref[0, c] = t_ref[0, c].reshape(2 * own, rows).T


def prepare(me, tokens, cotangent, slabs):
    rows, features = tokens.shape
    block = features // slabs
    own = block // 4
    whole = pl.BlockSpec((rows, features), lambda i, me: (0, 0))
    turned = pl.BlockSpec((1, 2, 2, own, rows), lambda i, me: (i, 0, 0, 0, 0))
    plain = pl.BlockSpec((1, 2, rows, 2 * own), lambda i, me: (i, 0, 0, 0))
    turned_shape = jax.ShapeDtypeStruct((slabs, 2, 2, own, rows), BF)
    plain_shape = jax.ShapeDtypeStruct((slabs, 2, rows, 2 * own), BF)
    return pl.pallas_call(
        prepare_body,
        grid_spec=pltpu.PrefetchScalarGridSpec(
            num_scalar_prefetch=1,
            grid=(slabs,),
            in_specs=[whole, whole],
            out_specs=[
                pl.BlockSpec((rows, block), lambda i, me: (0, i)),
                pl.BlockSpec((rows, HD), lambda i, me: (0, 0)),
                turned,
                plain,
                turned,
                plain,
            ],
            scratch_shapes=[pltpu.VMEM((rows, HD), F32)],
        ),
        out_shape=[
            jax.ShapeDtypeStruct((rows, features), F32),
            jax.ShapeDtypeStruct((rows, HD), F32),
            turned_shape,
            plain_shape,
            turned_shape,
            plain_shape,
        ],
        compiler_params=ARBITRARY,
        name="prepare",
    )(me, tokens, cotangent)


def distance(i):
    return (i + 1) // 2 * (1 if i % 2 == 0 else -1)


def project_kv_body(me_ref, x_ref, near_ref, near_far_ref, far_ref, far_far_ref, k_ref, kv_ref):
    slabs = x_ref.shape[0]
    rows, width = k_ref.shape
    close = near_ref.shape[0]
    for n in range(2 * width // 256):
        cols = slice(n * 256, (n + 1) * 256)
        acc = jnp.zeros((rows, 256), F32)
        for i in range(slabs):
            slab = lax.rem(me_ref[0] + slabs + distance(i), slabs)
            if i < close:
                pieces = near_ref[i, :, cols], near_far_ref[i, :, cols]
            else:
                pieces = far_ref[i - close, :, cols], far_far_ref[i - close, :, cols]
            for c, piece in enumerate(pieces):
                acc = acc + dot(x_ref[slab, c], piece)
        for j in range(2):
            at = n * 256 + j * HD
            part = acc[:, j * HD : (j + 1) * HD]
            if at < width:
                k_ref[:, at : at + HD] = part
                kv_ref[:rows, at : at + HD] = normalize(part)[0].astype(BF)
            else:
                kv_ref[rows:, at - width : at - width + HD] = part.astype(BF)


def project_kv(me, x, near, near_far, far, far_far):
    rows, width = x.shape[2], near.shape[2] // 2
    return pl.pallas_call(
        project_kv_body,
        in_specs=[pl.BlockSpec(memory_space=pltpu.SMEM)] + [pl.BlockSpec(memory_space=pltpu.VMEM)] * 5,
        out_shape=[
            jax.ShapeDtypeStruct((rows, width), F32),
            jax.ShapeDtypeStruct((2 * rows, width), BF),
        ],
        name="project_kv",
    )(me, x, near, near_far, far, far_far)


def project_qo_body(x_ref, c_ref, b_ref, by_ref, bc_ref, byc_ref, q_ref, g_ref):
    step = pl.program_id(0)
    width = q_ref.shape[1]
    mine = jnp.concatenate([b_ref[0], by_ref[0]], axis=0)
    theirs = jnp.concatenate([bc_ref[0], byc_ref[0]], axis=0)
    part = dot(x_ref[0, 0], mine[:, :width]) + dot(x_ref[0, 1], theirs[:, :width])
    part_g = dot(c_ref[0, 0], mine[:, width:]) + dot(c_ref[0, 1], theirs[:, width:])

    @pl.when(step == 0)
    def _():
        q_ref[...] = part
        g_ref[...] = part_g

    @pl.when(step > 0)
    def _():
        q_ref[...] += part
        g_ref[...] += part_g


def project_qo(x, c, *pieces):
    slabs, _, rows, depth = x.shape
    own, both = pieces[0].shape[1:]
    result = pl.BlockSpec((rows, both // 2), lambda i: (0, 0))
    return pl.pallas_call(
        project_qo_body,
        grid=(slabs,),
        in_specs=[pl.BlockSpec((1, 2, rows, depth), lambda i: (i, 0, 0, 0))] * 2
        + [pl.BlockSpec((1, own, both), lambda i: (i, 0, 0))] * 4,
        out_specs=[result, result],
        out_shape=[jax.ShapeDtypeStruct((rows, both // 2), F32)] * 2,
        compiler_params=ARBITRARY,
        name="project_qo",
    )(x, c, *pieces)


def attend_body(q_ref, g_ref, kv_ref, att_ref, qb_ref, dkv_ref, e_ref):
    blocks = kv_ref.shape[0]
    rows = q_ref.shape[0]
    keys = kv_ref.shape[2]
    scale = HD ** (-0.5)
    q_unit, q_inv = normalize(q_ref[...])
    q = q_unit.astype(BF)
    g = g_ref[...].astype(BF)
    total = jnp.zeros((8, rows), F32)
    att_t = jnp.zeros((HD, rows), F32)
    for j in range(blocks):
        e = jnp.exp(dot(kv_ref[j, 0], q, 1, 1) * scale)
        e_ref[j] = e
        total = total + jnp.sum(e.reshape(keys // 8, 8, rows), axis=0)
        att_t = att_t + dot(kv_ref[j, 1].T, e.astype(BF))
    total = jnp.sum(total, axis=0, keepdims=True)
    inv_total = 1.0 / total
    att = (att_t * inv_total).T.astype(BF)
    att_ref[...] = att
    delta = jnp.sum((g.astype(F32) * att.astype(F32)).T, axis=0, keepdims=True)
    dq_t = jnp.zeros((HD, rows), F32)
    for j in range(blocks):
        p = e_ref[j] * inv_total
        dp = dot(kv_ref[j, 1], g, 1, 1)
        ds = (p * ((dp - delta) * scale)).astype(BF)
        dkv_ref[j, 0] = dot(ds, q).astype(BF)
        dkv_ref[j, 1] = dot(p.astype(BF), g).astype(BF)
        dq_t = dq_t + dot(kv_ref[j, 0].T, ds)
    qb_ref[...] = normalize_back(dq_t.T, q_unit, q_inv).astype(BF)


def attend(q, g, kv):
    rows, width = q.shape
    blocks, _, keys, _ = kv.shape
    row_spec = pl.BlockSpec((rows, HD), lambda h: (0, h))
    kv_spec = pl.BlockSpec((blocks, 2, keys, HD), lambda h: (0, 0, 0, h))
    return pl.pallas_call(
        attend_body,
        grid=(width // HD,),
        in_specs=[row_spec, row_spec, kv_spec],
        out_specs=[row_spec, row_spec, kv_spec],
        out_shape=[
            jax.ShapeDtypeStruct((rows, width), BF),
            jax.ShapeDtypeStruct((rows, width), BF),
            jax.ShapeDtypeStruct(kv.shape, BF),
        ],
        scratch_shapes=[pltpu.VMEM((blocks, keys, rows), F32)],
        compiler_params=pltpu.CompilerParams(dimension_semantics=("arbitrary",)),
        name="attend",
    )(q, g, kv)


def key_back_body(s_ref, k_ref, kb_ref, vb_ref):
    rows, width = k_ref.shape
    for h in range(width // HD):
        cols = slice(h * HD, (h + 1) * HD)
        unit, inv = normalize(k_ref[:, cols])
        kb_ref[:, cols] = normalize_back(s_ref[:rows, cols].astype(F32), unit, inv).astype(BF)
    vb_ref[...] = s_ref[rows:, :]


def key_back(summed, k):
    return pl.pallas_call(
        key_back_body,
        out_shape=[jax.ShapeDtypeStruct(k.shape, BF)] * 2,
        name="key_back",
    )(summed, k)


def terms_body(x_ref, c_ref, a_ref, b_ref, send_ref, keep_ref, *, split):
    own, rows = x_ref.shape[3:]
    width = a_ref.shape[1]
    left = x_ref[0].reshape(4 * own, rows)
    first = dot(left, a_ref[...]).astype(BF)
    left = c_ref[0].reshape(4 * own, rows)
    other = dot(left, b_ref[...]).astype(BF)
    for c, out_ref in enumerate((keep_ref, send_ref)):
        for y in range(2):
            at = (2 * c + y) * own
            spot = (y, 0) if split else (0, y)
            out_ref[spot[0], spot[1], :, :width] = first[at : at + own]
            out_ref[spot[0], spot[1], :, width:] = other[at : at + own]


def terms(x_t, c_t, a, b, split):
    slabs, _, _, own, rows = x_t.shape
    width = a.shape[1]
    slab = pl.BlockSpec((1, 2, 2, own, rows), lambda i: (i, 0, 0, 0, 0))
    whole = pl.BlockSpec((rows, width), lambda i: (0, 0))
    if split:
        shape = (2, slabs, own, 2 * width)
        out = pl.BlockSpec((2, 1, own, 2 * width), lambda i: (0, i, 0, 0))
    else:
        shape = (slabs, 2, own, 2 * width)
        out = pl.BlockSpec((1, 2, own, 2 * width), lambda i: (i, 0, 0, 0))
    return pl.pallas_call(
        lambda *refs: terms_body(*refs, split=split),
        grid=(slabs,),
        in_specs=[slab, slab, whole, whole],
        out_specs=[out, out],
        out_shape=[jax.ShapeDtypeStruct(shape, BF)] * 2,
        compiler_params=ARBITRARY,
        name="terms_split" if split else "terms_plain",
    )(x_t, c_t, a, b)


def merge_body(half_ref, y_ref, keep_ref, got_ref, out_ref):
    own = half_ref.shape[2]
    out_ref[0, :own] = (half_ref[0, 0].astype(F32) + y_ref[0].astype(F32)).astype(BF)
    for y in range(2):
        total = keep_ref[0, y].astype(F32) + got_ref[0, y].astype(F32)
        out_ref[0, (1 + y) * own : (2 + y) * own] = total.astype(BF)


def merge(half, from_y, keep, got):
    slabs, own, both = from_y.shape
    pair = pl.BlockSpec((1, 2, own, both), lambda i: (i, 0, 0, 0))
    return pl.pallas_call(
        merge_body,
        grid=(slabs,),
        in_specs=[
            pl.BlockSpec((1, 1, own, both), lambda i: (0, i, 0, 0)),
            pl.BlockSpec((1, own, both), lambda i: (i, 0, 0)),
            pair,
            pair,
        ],
        out_specs=pl.BlockSpec((1, 3 * own, both), lambda i: (i, 0, 0)),
        out_shape=jax.ShapeDtypeStruct((slabs, 3 * own, both), BF),
        compiler_params=ARBITRARY,
        name="merge",
    )(half, from_y, keep, got)


def inner_body(
    me_ref, qb_ref, kb_ref, vb_ref, near_ref, near_far_ref, far_ref, far_far_ref,
    b_ref, by_ref, bc_ref, byc_ref, unit_ref, out_ref, sum_ref, both_ref, w_ref, *, close,
):
    step = pl.program_id(0)
    own = b_ref.shape[1]
    width = qb_ref.shape[1]
    away_y, away_c = me_ref[2], me_ref[1]
    for y, c, ref in ((0, 0, b_ref), (1, 0, by_ref), (0, 1, bc_ref), (1, 1, byc_ref)):
        w_ref[lax.rem(away_y + y, 2), lax.rem(away_c + c, 2), :, :width] = ref[0, :, :width]

    def place(refs):
        for c, ref in enumerate(refs):
            for y in range(2):
                spot = lax.rem(away_y + y, 2), lax.rem(away_c + c, 2)
                w_ref[spot[0], spot[1], :, width:] = ref[0, y * own : (y + 1) * own]

    @pl.when(step < close)
    def _():
        place((near_ref, near_far_ref))

    @pl.when(step >= close)
    def _():
        place((far_ref, far_far_ref))

    low = jnp.concatenate([qb_ref[...], kb_ref[...], vb_ref[...]], axis=1)
    result = dot(low, w_ref[...].reshape(4 * own, 3 * width), 1, 1)
    out_ref[0] = result.astype(BF)
    both = result * unit_ref[...]
    lanes = range(0, result.shape[1], HD)
    plain = sum(result[:, i : i + HD] for i in lanes)
    times = sum(both[:, i : i + HD] for i in lanes)

    @pl.when(step == 0)
    def _():
        sum_ref[...] = plain
        both_ref[...] = times

    @pl.when(step > 0)
    def _():
        sum_ref[...] += plain
        both_ref[...] += times


def inner(me, qb, kb, vb, near, near_far, far, far_far, pieces, unit):
    rows, width = qb.shape
    slabs, own, both = pieces[0].shape
    close = near.shape[0]

    def place(i, me):
        sign = 1 - 2 * lax.rem(i, 2)
        return lax.rem(me[0] + slabs + lax.div(i + 1, 2) * sign, slabs)

    whole = pl.BlockSpec((rows, width), lambda i, me: (0, 0))
    stat = pl.BlockSpec((rows, HD), lambda i, me: (0, 0))
    first = pl.BlockSpec((1, 2 * own, both), lambda i, me: (jnp.minimum(i, close - 1), 0, 0))
    last = pl.BlockSpec((1, 2 * own, both), lambda i, me: (jnp.maximum(i - close, 0), 0, 0))
    return pl.pallas_call(
        lambda *refs: inner_body(*refs, close=close),
        grid_spec=pltpu.PrefetchScalarGridSpec(
            num_scalar_prefetch=1,
            grid=(slabs,),
            in_specs=[whole, whole, whole, first, first, last, last]
            + [pl.BlockSpec((1, own, both), lambda i, me: (place(i, me), 0, 0))] * 4
            + [pl.BlockSpec((rows, 4 * own), lambda i, me: (0, place(i, me)))],
            out_specs=[
                pl.BlockSpec((1, rows, 4 * own), lambda i, me: (place(i, me), 0, 0)),
                stat,
                stat,
            ],
            scratch_shapes=[pltpu.VMEM((2, 2, own, 3 * width), BF)],
        ),
        out_shape=[
            jax.ShapeDtypeStruct((slabs, rows, 4 * own), BF),
            jax.ShapeDtypeStruct((rows, HD), F32),
            jax.ShapeDtypeStruct((rows, HD), F32),
        ],
        compiler_params=ARBITRARY,
        name="inner",
    )(me, qb, kb, vb, near, near_far, far, far_far, *pieces, unit)


def swap(value, axis):
    return lax.ppermute(value, axis, [(0, 1), (1, 0)])


def plus(a, b):
    return (a.astype(F32) + b.astype(F32)).astype(BF)


def ring_gather(value):
    size = lax.axis_size("seq")
    up = [(i, (i + 1) % size) for i in range(size)]
    down = [(i, (i - 1) % size) for i in range(size)]
    half = value.shape[0] // 2
    rows = [value]
    high = low = value
    for _ in range(size // 2 - 1):
        high = lax.ppermute(high, "seq", up)
        low = lax.ppermute(low, "seq", down)
        rows += [high, low]
    high = lax.ppermute(high[:half], "seq", up)
    low = lax.ppermute(low[half:], "seq", down)
    return rows + [jnp.concatenate([high, low], axis=0)]


def pieces_of(value):
    parts = []
    for _ in range(3):
        part = lax.reduce_precision(value, 8, 7)
        parts.append(part.astype(BF))
        value = value - part
    return parts


def local(tokens, cotangent, qkv_weight, out_weight):
    row_count, feature_count = tokens.shape[1:]
    own, _, width = qkv_weight.shape
    slabs = lax.axis_size("seq")
    shares = lax.axis_size(("x", "yhi"))
    me = jnp.stack([lax.axis_index("seq"), lax.axis_index("core"), lax.axis_index("ylo")]).astype(jnp.int32)
    kv_weight = qkv_weight[:, 1:].reshape(own, 2 * width)
    qo_weight = jnp.concatenate([qkv_weight[:, 0], out_weight], axis=1)
    kv_weight = jnp.concatenate([kv_weight, swap(kv_weight, "ylo")], axis=0)
    qo_mine = lax.all_gather(qo_weight, "seq")
    unit, inverse, x_t, x_r, c_t, c_r = prepare(me, tokens[0], cotangent[0], slabs)
    kv_weight, x_r = lax.optimization_barrier((kv_weight, x_r))
    ring = ring_gather(kv_weight)
    near, far = jnp.stack(ring[:5]), jnp.stack(ring[5:])
    near_far, far_far = swap(near, "core"), swap(far, "core")
    key, key_value = project_kv(me, x_r, near, near_far, far, far_far)
    every = lax.all_gather(key_value, "seq", axis=0, tiled=True)
    qo_y = swap(qo_mine, "ylo")
    qo_pieces = (qo_mine, qo_y, swap(qo_mine, "core"), swap(qo_y, "core"))
    query, grad_rows = project_qo(x_r, c_r, *qo_pieces)
    attended, query_back, pair = attend(
        query, grad_rows, every.reshape(slabs, 2, row_count, width)
    )
    pair = lax.psum_scatter(
        pair.reshape(slabs * 2 * row_count, width), "seq", scatter_dimension=0, tiled=True
    )
    send, keep = terms(x_t, c_t, query_back, attended, True)
    half = plus(keep, swap(send, "core"))
    from_y = swap(half[1], "ylo")
    key, from_y = lax.optimization_barrier((key, from_y))
    key_grad, value_grad = key_back(pair, key)
    send, keep = terms(x_t, x_t, key_grad, value_grad, False)
    merged = merge(half, from_y, keep, swap(send, "core"))
    merged = lax.psum_scatter(
        merged.reshape(slabs * 3 * own, 2 * width), "seq", scatter_dimension=0, tiled=True
    )
    query_out = merged[:own].astype(F32)
    key_value_grad = merged[own : 2 * own].astype(F32) + swap(merged[2 * own :], "ylo").astype(F32)
    share, plain, both = inner(
        me, query_back, key_grad, value_grad, near, near_far, far, far_far, qo_pieces, unit
    )
    stats = jnp.stack(pieces_of(jnp.sum(plain, axis=1)) + pieces_of(jnp.sum(both, axis=1)))
    stats = stats.reshape(-1, share.shape[2])
    stats = jnp.pad(stats, ((0, 16 - stats.shape[0]), (0, 0)))
    load = jnp.concatenate([share, jnp.broadcast_to(stats, (shares, *stats.shape))], axis=1)
    load = lax.all_to_all(load, ("x", "yhi"), 0, 0, tiled=True).astype(F32)
    load = jnp.sum(load, axis=0)
    own_share = load[:row_count]
    totals = load[row_count:].reshape(-1)[: 6 * row_count].reshape(2, 3, row_count)
    totals = jnp.sum(totals, axis=1)[:, :, None] / feature_count
    offset = lax.axis_index(("x", "yhi")) * share.shape[2]
    unit_own = lax.dynamic_slice_in_dim(unit, offset, share.shape[2], 1)
    branch = (own_share - totals[0] - unit_own * totals[1]) * inverse[:, :1]
    qkv_grad = jnp.stack(
        [query_out[:, :width], key_value_grad[:, :width], key_value_grad[:, width:]], axis=1
    )
    return (qkv_grad, query_out[:, width:], branch.astype(BF)[None])


def solution(mesh):
    split = jax.sharding.Mesh(
        mesh.devices.reshape(mesh.shape["seq"], mesh.shape["tensor"] // 2, 2, 2, 2),
        ("seq", "x", "yhi", "ylo", "core"),
    )
    blocks = ("seq", "ylo", "core")
    heads = ("x", "yhi")
    return jax.shard_map(
        local,
        mesh=split,
        in_specs=(
            P(("ylo", "core"), "seq", None),
            P(("ylo", "core"), "seq", None),
            P(blocks, None, heads),
            P(blocks, heads),
        ),
        out_specs=(
            P(blocks, None, heads),
            P(blocks, heads),
            P(("ylo", "core"), "seq", heads),
        ),
        check_vma=False,
    )
```

```python
import jax
import jax.numpy as jnp
from jax import lax
from jax.experimental import pallas as pl
from jax.experimental.pallas import tpu as pltpu
from jax.sharding import PartitionSpec as P

HD = 128
epsilon = 1e-06
BF = jnp.bfloat16
F32 = jnp.float32


def dot(a, b, ca=1, cb=0):
    return lax.dot_general(a, b, (((ca,), (cb,)), ((), ())), preferred_element_type=F32)


def normalize(values, axis=-1):
    average = jnp.mean(values, axis=axis, keepdims=True)
    centered = values - average
    inverse = lax.rsqrt(jnp.mean(centered * centered, axis=axis, keepdims=True) + epsilon)
    return (centered * inverse, inverse)


def normalize_back(gradient, normed, inverse, axis=-1):
    mean_grad = jnp.mean(gradient, axis=axis, keepdims=True)
    mean_both = jnp.mean(gradient * normed, axis=axis, keepdims=True)
    return (gradient - mean_grad - normed * mean_both) * inverse


ARBITRARY = pltpu.CompilerParams(dimension_semantics=("arbitrary",))


def prepare_body(me_ref, tok_ref, cot_ref, unit_ref, inv_ref, xt_ref, xr_ref, ct_ref, cr_ref, mean_ref):
    step = pl.program_id(0)
    rows = tok_ref.shape[0]
    block = unit_ref.shape[1]
    own = block // 4

    @pl.when(step == 0)
    def _():
        values = tok_ref[...].astype(F32)
        average = jnp.mean(values, axis=-1, keepdims=True)
        centered = values - average
        inverse = lax.rsqrt(jnp.mean(centered * centered, axis=-1, keepdims=True) + epsilon)
        mean_ref[...] = jnp.broadcast_to(average, (rows, HD))
        inv_ref[...] = jnp.broadcast_to(inverse, (rows, HD))

    here = pl.ds(pl.multiple_of(step * block, HD), block)
    unit = (tok_ref[:, here].astype(F32) - mean_ref[:, :1]) * inv_ref[:, :1]
    unit_ref[...] = unit
    for value, t_ref, r_ref in (
        (unit.astype(BF), xt_ref, xr_ref),
        (cot_ref[:, here], ct_ref, cr_ref),
    ):
        turned = value.T
        for y in range(2):
            for c in range(2):
                away_y, away_c = lax.rem(me_ref[2] + y, 2), lax.rem(me_ref[1] + c, 2)
                at = (2 * y + c) * own
                t_ref[0, away_c, away_y] = turned[at : at + own]
        for c in range(2):
            r_ref[0, c] = t_ref[0, c].reshape(2 * own, rows).T


def prepare(me, tokens, cotangent, slabs):
    rows, features = tokens.shape
    block = features // slabs
    own = block // 4
    whole = pl.BlockSpec((rows, features), lambda i, me: (0, 0))
    turned = pl.BlockSpec((1, 2, 2, own, rows), lambda i, me: (i, 0, 0, 0, 0))
    plain = pl.BlockSpec((1, 2, rows, 2 * own), lambda i, me: (i, 0, 0, 0))
    turned_shape = jax.ShapeDtypeStruct((slabs, 2, 2, own, rows), BF)
    plain_shape = jax.ShapeDtypeStruct((slabs, 2, rows, 2 * own), BF)
    return pl.pallas_call(
        prepare_body,
        grid_spec=pltpu.PrefetchScalarGridSpec(
            num_scalar_prefetch=1,
            grid=(slabs,),
            in_specs=[whole, whole],
            out_specs=[
                pl.BlockSpec((rows, block), lambda i, me: (0, i)),
                pl.BlockSpec((rows, HD), lambda i, me: (0, 0)),
                turned,
                plain,
                turned,
                plain,
            ],
            scratch_shapes=[pltpu.VMEM((rows, HD), F32)],
        ),
        out_shape=[
            jax.ShapeDtypeStruct((rows, features), F32),
            jax.ShapeDtypeStruct((rows, HD), F32),
            turned_shape,
            plain_shape,
            turned_shape,
            plain_shape,
        ],
        compiler_params=ARBITRARY,
        name="prepare",
    )(me, tokens, cotangent)


def distance(i):
    return (i + 1) // 2 * (1 if i % 2 == 0 else -1)


def project_kv_body(me_ref, x_ref, near_ref, near_far_ref, far_ref, far_far_ref, k_ref, kv_ref):
    slabs = x_ref.shape[0]
    rows, width = k_ref.shape
    close = near_ref.shape[0]
    for n in range(2 * width // 256):
        cols = slice(n * 256, (n + 1) * 256)
        acc = jnp.zeros((rows, 256), F32)
        for i in range(slabs):
            slab = lax.rem(me_ref[0] + slabs + distance(i), slabs)
            if i < close:
                pieces = near_ref[i, :, cols], near_far_ref[i, :, cols]
            else:
                pieces = far_ref[i - close, :, cols], far_far_ref[i - close, :, cols]
            for c, piece in enumerate(pieces):
                acc = acc + dot(x_ref[slab, c], piece)
        for j in range(2):
            at = n * 256 + j * HD
            part = acc[:, j * HD : (j + 1) * HD]
            if at < width:
                k_ref[:, at : at + HD] = part
                kv_ref[:rows, at : at + HD] = normalize(part)[0].astype(BF)
            else:
                kv_ref[rows:, at - width : at - width + HD] = part.astype(BF)


def project_kv(me, x, near, near_far, far, far_far):
    rows, width = x.shape[2], near.shape[2] // 2
    return pl.pallas_call(
        project_kv_body,
        in_specs=[pl.BlockSpec(memory_space=pltpu.SMEM)] + [pl.BlockSpec(memory_space=pltpu.VMEM)] * 5,
        out_shape=[
            jax.ShapeDtypeStruct((rows, width), F32),
            jax.ShapeDtypeStruct((2 * rows, width), BF),
        ],
        name="project_kv",
    )(me, x, near, near_far, far, far_far)


def project_qo_body(x_ref, c_ref, b_ref, by_ref, bc_ref, byc_ref, q_ref, g_ref):
    step = pl.program_id(0)
    width = q_ref.shape[1]
    mine = jnp.concatenate([b_ref[0], by_ref[0]], axis=0)
    theirs = jnp.concatenate([bc_ref[0], byc_ref[0]], axis=0)
    part = dot(x_ref[0, 0], mine[:, :width]) + dot(x_ref[0, 1], theirs[:, :width])
    part_g = dot(c_ref[0, 0], mine[:, width:]) + dot(c_ref[0, 1], theirs[:, width:])

    @pl.when(step == 0)
    def _():
        q_ref[...] = part
        g_ref[...] = part_g

    @pl.when(step > 0)
    def _():
        q_ref[...] += part
        g_ref[...] += part_g


def project_qo(x, c, *pieces):
    slabs, _, rows, depth = x.shape
    own, both = pieces[0].shape[1:]
    result = pl.BlockSpec((rows, both // 2), lambda i: (0, 0))
    return pl.pallas_call(
        project_qo_body,
        grid=(slabs,),
        in_specs=[pl.BlockSpec((1, 2, rows, depth), lambda i: (i, 0, 0, 0))] * 2
        + [pl.BlockSpec((1, own, both), lambda i: (i, 0, 0))] * 4,
        out_specs=[result, result],
        out_shape=[jax.ShapeDtypeStruct((rows, both // 2), F32)] * 2,
        compiler_params=ARBITRARY,
        name="project_qo",
    )(x, c, *pieces)


def attend_body(q_ref, g_ref, kv_ref, att_ref, qb_ref, dkv_ref, e_ref):
    blocks = kv_ref.shape[0]
    rows = q_ref.shape[0]
    keys = kv_ref.shape[2]
    scale = HD ** (-0.5)
    q_unit, q_inv = normalize(q_ref[...])
    q = q_unit.astype(BF)
    g = g_ref[...].astype(BF)
    total = jnp.zeros((8, rows), F32)
    att_t = jnp.zeros((HD, rows), F32)
    for j in range(blocks):
        e = jnp.exp(dot(kv_ref[j, 0], q, 1, 1) * scale)
        e_ref[j] = e
        total = total + jnp.sum(e.reshape(keys // 8, 8, rows), axis=0)
        att_t = att_t + dot(kv_ref[j, 1].T, e.astype(BF))
    total = jnp.sum(total, axis=0, keepdims=True)
    inv_total = 1.0 / total
    att = (att_t * inv_total).T.astype(BF)
    att_ref[...] = att
    delta = jnp.sum((g.astype(F32) * att.astype(F32)).T, axis=0, keepdims=True)
    dq_t = jnp.zeros((HD, rows), F32)
    for j in range(blocks):
        p = e_ref[j] * inv_total
        dp = dot(kv_ref[j, 1], g, 1, 1)
        ds = (p * ((dp - delta) * scale)).astype(BF)
        dkv_ref[j, 0] = dot(ds, q).astype(BF)
        dkv_ref[j, 1] = dot(p.astype(BF), g).astype(BF)
        dq_t = dq_t + dot(kv_ref[j, 0].T, ds)
    qb_ref[...] = normalize_back(dq_t.T, q_unit, q_inv).astype(BF)


def attend(q, g, kv):
    rows, width = q.shape
    blocks, _, keys, _ = kv.shape
    row_spec = pl.BlockSpec((rows, HD), lambda h: (0, h))
    kv_spec = pl.BlockSpec((blocks, 2, keys, HD), lambda h: (0, 0, 0, h))
    return pl.pallas_call(
        attend_body,
        grid=(width // HD,),
        in_specs=[row_spec, row_spec, kv_spec],
        out_specs=[row_spec, row_spec, kv_spec],
        out_shape=[
            jax.ShapeDtypeStruct((rows, width), BF),
            jax.ShapeDtypeStruct((rows, width), BF),
            jax.ShapeDtypeStruct(kv.shape, BF),
        ],
        scratch_shapes=[pltpu.VMEM((blocks, keys, rows), F32)],
        compiler_params=pltpu.CompilerParams(dimension_semantics=("arbitrary",)),
        name="attend",
    )(q, g, kv)


def key_back_body(s_ref, k_ref, kb_ref, vb_ref):
    rows, width = k_ref.shape
    for h in range(width // HD):
        cols = slice(h * HD, (h + 1) * HD)
        unit, inv = normalize(k_ref[:, cols])
        kb_ref[:, cols] = normalize_back(s_ref[:rows, cols].astype(F32), unit, inv).astype(BF)
    vb_ref[...] = s_ref[rows:, :]


def key_back(summed, k):
    return pl.pallas_call(
        key_back_body,
        out_shape=[jax.ShapeDtypeStruct(k.shape, BF)] * 2,
        name="key_back",
    )(summed, k)


def terms_body(x_ref, c_ref, a_ref, b_ref, *refs, split, add):
    own, rows = x_ref.shape[3:]
    width = a_ref.shape[1]
    first = dot(x_ref[0, 0].reshape(2 * own, rows), a_ref[...])
    other = dot(c_ref[0, 0].reshape(2 * own, rows), b_ref[...])
    if add:
        got_ref = refs[0]
        refs = refs[1:]
    for y in range(2):
        here = slice(y * own, (y + 1) * own)
        spot = (y, 0) if split else (0, y)
        for cols, value in ((slice(None, width), first), (slice(width, None), other)):
            value = value[here]
            if add:
                value = value + got_ref[spot[0], spot[1], :, cols].astype(F32)
            if not add:
                refs[0][spot[0], spot[1], :, cols] = value.astype(BF)
            elif split:
                refs[y][0, :, cols] = value.astype(BF)
            else:
                refs[2][0, (1 + y) * own : (2 + y) * own, cols] = value.astype(BF)
    if add and not split:
        total = refs[0][0].astype(F32) + refs[1][0].astype(F32)
        refs[2][0, :own] = total.astype(BF)


def terms(x_t, c_t, a, b, split, got=None, extra=()):
    slabs, _, _, own, rows = x_t.shape
    width = a.shape[1]
    add = got is not None
    core = 0 if add else 1
    slab = pl.BlockSpec((1, 1, 2, own, rows), lambda i: (i, core, 0, 0, 0))
    whole = pl.BlockSpec((rows, width), lambda i: (0, 0))
    if split:
        shape = (2, slabs, own, 2 * width)
        block = pl.BlockSpec((2, 1, own, 2 * width), lambda i: (0, i, 0, 0))
    else:
        shape = (slabs, 2, own, 2 * width)
        block = pl.BlockSpec((1, 2, own, 2 * width), lambda i: (i, 0, 0, 0))
    piece = pl.BlockSpec((1, own, 2 * width), lambda i: (i, 0, 0))
    if not add:
        specs, outs, shapes = [], block, shape
    elif split:
        specs, outs, shapes = [block], [piece, piece], [shape[1:]] * 2
    else:
        specs, shapes = [block, piece, piece], (slabs, 3 * own, 2 * width)
        outs = pl.BlockSpec((1, 3 * own, 2 * width), lambda i: (i, 0, 0))
    make = lambda v: jax.ShapeDtypeStruct(v, BF)
    return pl.pallas_call(
        lambda *refs: terms_body(*refs, split=split, add=add),
        grid=(slabs,),
        in_specs=[slab, slab, whole, whole] + specs,
        out_specs=outs,
        out_shape=[make(v) for v in shapes] if isinstance(shapes, list) else make(shapes),
        compiler_params=ARBITRARY,
        name="terms" + ("_split" if split else "_plain") + ("_add" if add else "_send"),
    )(x_t, c_t, a, b, *(() if got is None else (got,)), *extra)


def inner_body(
    me_ref, qb_ref, kb_ref, vb_ref, near_ref, near_far_ref, far_ref, far_far_ref,
    b_ref, by_ref, bc_ref, byc_ref, unit_ref, out_ref, sum_ref, both_ref, w_ref, *, close,
):
    step = pl.program_id(0)
    own = b_ref.shape[1]
    width = qb_ref.shape[1]
    away_y, away_c = me_ref[2], me_ref[1]
    for y, c, ref in ((0, 0, b_ref), (1, 0, by_ref), (0, 1, bc_ref), (1, 1, byc_ref)):
        w_ref[lax.rem(away_y + y, 2), lax.rem(away_c + c, 2), :, :width] = ref[0, :, :width]

    def place(refs):
        for c, ref in enumerate(refs):
            for y in range(2):
                spot = lax.rem(away_y + y, 2), lax.rem(away_c + c, 2)
                w_ref[spot[0], spot[1], :, width:] = ref[0, y * own : (y + 1) * own]

    @pl.when(step < close)
    def _():
        place((near_ref, near_far_ref))

    @pl.when(step >= close)
    def _():
        place((far_ref, far_far_ref))

    low = jnp.concatenate([qb_ref[...], kb_ref[...], vb_ref[...]], axis=1)
    result = dot(low, w_ref[...].reshape(4 * own, 3 * width), 1, 1)
    out_ref[0] = result.astype(BF)
    both = result * unit_ref[...]
    lanes = range(0, result.shape[1], HD)
    plain = sum(result[:, i : i + HD] for i in lanes)
    times = sum(both[:, i : i + HD] for i in lanes)

    @pl.when(step == 0)
    def _():
        sum_ref[...] = plain
        both_ref[...] = times

    @pl.when(step > 0)
    def _():
        sum_ref[...] += plain
        both_ref[...] += times


def inner(me, qb, kb, vb, near, near_far, far, far_far, pieces, unit):
    rows, width = qb.shape
    slabs, own, both = pieces[0].shape
    close = near.shape[0]

    def place(i, me):
        sign = 1 - 2 * lax.rem(i, 2)
        return lax.rem(me[0] + slabs + lax.div(i + 1, 2) * sign, slabs)

    whole = pl.BlockSpec((rows, width), lambda i, me: (0, 0))
    stat = pl.BlockSpec((rows, HD), lambda i, me: (0, 0))
    first = pl.BlockSpec((1, 2 * own, both), lambda i, me: (jnp.minimum(i, close - 1), 0, 0))
    last = pl.BlockSpec((1, 2 * own, both), lambda i, me: (jnp.maximum(i - close, 0), 0, 0))
    return pl.pallas_call(
        lambda *refs: inner_body(*refs, close=close),
        grid_spec=pltpu.PrefetchScalarGridSpec(
            num_scalar_prefetch=1,
            grid=(slabs,),
            in_specs=[whole, whole, whole, first, first, last, last]
            + [pl.BlockSpec((1, own, both), lambda i, me: (place(i, me), 0, 0))] * 4
            + [pl.BlockSpec((rows, 4 * own), lambda i, me: (0, place(i, me)))],
            out_specs=[
                pl.BlockSpec((1, rows, 4 * own), lambda i, me: (place(i, me), 0, 0)),
                stat,
                stat,
            ],
            scratch_shapes=[pltpu.VMEM((2, 2, own, 3 * width), BF)],
        ),
        out_shape=[
            jax.ShapeDtypeStruct((slabs, rows, 4 * own), BF),
            jax.ShapeDtypeStruct((rows, HD), F32),
            jax.ShapeDtypeStruct((rows, HD), F32),
        ],
        compiler_params=ARBITRARY,
        name="inner",
    )(me, qb, kb, vb, near, near_far, far, far_far, *pieces, unit)


def swap(value, axis):
    return lax.ppermute(value, axis, [(0, 1), (1, 0)])


def plus(a, b):
    return (a.astype(F32) + b.astype(F32)).astype(BF)


def ring_gather(value, held):
    size = lax.axis_size("seq")
    up = [(i, (i + 1) % size) for i in range(size)]
    down = [(i, (i - 1) % size) for i in range(size)]
    half = value.shape[0] // 2
    rows = [value]
    high = low = value
    for step in range(size // 2 - 1):
        high = lax.ppermute(high, "seq", up)
        low = lax.ppermute(low, "seq", down)
        if step == 0:
            high, low, held = lax.optimization_barrier((high, low, held))
        rows += [high, low]
    high = lax.ppermute(high[:half], "seq", up)
    low = lax.ppermute(low[half:], "seq", down)
    return rows + [jnp.concatenate([high, low], axis=0)], held


def pieces_of(value):
    parts = []
    for _ in range(3):
        part = lax.reduce_precision(value, 8, 7)
        parts.append(part.astype(BF))
        value = value - part
    return parts


def local(tokens, cotangent, qkv_weight, out_weight):
    row_count, feature_count = tokens.shape[1:]
    own, _, width = qkv_weight.shape
    slabs = lax.axis_size("seq")
    shares = lax.axis_size(("x", "yhi"))
    me = jnp.stack([lax.axis_index("seq"), lax.axis_index("core"), lax.axis_index("ylo")]).astype(jnp.int32)
    kv_weight = qkv_weight[:, 1:].reshape(own, 2 * width)
    qo_weight = jnp.concatenate([qkv_weight[:, 0], out_weight], axis=1)
    kv_weight = jnp.concatenate([kv_weight, swap(kv_weight, "ylo")], axis=0)
    qo_mine = lax.all_gather(qo_weight, "seq")
    unit, inverse, x_t, x_r, c_t, c_r = prepare(me, tokens[0], cotangent[0], slabs)
    ring, x_r = ring_gather(kv_weight, x_r)
    near, far = jnp.stack(ring[:5]), jnp.stack(ring[5:])
    near_far, far_far = swap(near, "core"), swap(far, "core")
    key, key_value = project_kv(me, x_r, near, near_far, far, far_far)
    every = lax.all_gather(key_value, "seq", axis=0, tiled=True)
    qo_y = swap(qo_mine, "ylo")
    qo_pieces = (qo_mine, qo_y, swap(qo_mine, "core"), swap(qo_y, "core"))
    query, grad_rows = project_qo(x_r, c_r, *qo_pieces)
    attended, query_back, pair = attend(
        query, grad_rows, every.reshape(slabs, 2, row_count, width)
    )
    pair = lax.psum_scatter(
        pair.reshape(slabs * 2 * row_count, width), "seq", scatter_dimension=0, tiled=True
    )
    got = swap(terms(x_t, c_t, query_back, attended, True), "core")
    stay, go = terms(x_t, c_t, query_back, attended, True, got)
    from_y = swap(go, "ylo")
    key, from_y = lax.optimization_barrier((key, from_y))
    key_grad, value_grad = key_back(pair, key)
    got = swap(terms(x_t, x_t, key_grad, value_grad, False), "core")
    merged = terms(x_t, x_t, key_grad, value_grad, False, got, (stay, from_y))
    merged, key_grad = lax.optimization_barrier((merged, key_grad))
    merged = lax.psum_scatter(
        merged.reshape(slabs * 3 * own, 2 * width), "seq", scatter_dimension=0, tiled=True
    )
    query_out = merged[:own].astype(F32)
    key_value_grad = merged[own : 2 * own].astype(F32) + swap(merged[2 * own :], "ylo").astype(F32)
    share, plain, both = inner(
        me, query_back, key_grad, value_grad, near, near_far, far, far_far, qo_pieces, unit
    )
    stats = jnp.stack(pieces_of(jnp.sum(plain, axis=1)) + pieces_of(jnp.sum(both, axis=1)))
    stats = stats.reshape(-1, share.shape[2])
    stats = jnp.pad(stats, ((0, 16 - stats.shape[0]), (0, 0)))
    load = jnp.concatenate([share, jnp.broadcast_to(stats, (shares, *stats.shape))], axis=1)
    load = lax.all_to_all(load, ("x", "yhi"), 0, 0, tiled=True).astype(F32)
    load = jnp.sum(load, axis=0)
    own_share = load[:row_count]
    totals = load[row_count:].reshape(-1)[: 6 * row_count].reshape(2, 3, row_count)
    totals = jnp.sum(totals, axis=1)[:, :, None] / feature_count
    offset = lax.axis_index(("x", "yhi")) * share.shape[2]
    unit_own = lax.dynamic_slice_in_dim(unit, offset, share.shape[2], 1)
    branch = (own_share - totals[0] - unit_own * totals[1]) * inverse[:, :1]
    qkv_grad = jnp.stack(
        [query_out[:, :width], key_value_grad[:, :width], key_value_grad[:, width:]], axis=1
    )
    return (qkv_grad, query_out[:, width:], branch.astype(BF)[None])


def solution(mesh):
    split = jax.sharding.Mesh(
        mesh.devices.reshape(mesh.shape["seq"], mesh.shape["tensor"] // 2, 2, 2, 2),
        ("seq", "x", "yhi", "ylo", "core"),
    )
    blocks = ("seq", "ylo", "core")
    heads = ("x", "yhi")
    return jax.shard_map(
        local,
        mesh=split,
        in_specs=(
            P(("ylo", "core"), "seq", None),
            P(("ylo", "core"), "seq", None),
            P(blocks, None, heads),
            P(blocks, heads),
        ),
        out_specs=(
            P(blocks, None, heads),
            P(blocks, heads),
            P(("ylo", "core"), "seq", heads),
        ),
        check_vma=False,
    )
```

```python
import jax
import jax.numpy as jnp
from jax import lax
from jax.experimental import pallas as pl
from jax.experimental.pallas import tpu as pltpu
from jax.sharding import PartitionSpec as P

HD = 128
epsilon = 1e-06
BF = jnp.bfloat16
F32 = jnp.float32


def dot(a, b, ca=1, cb=0):
    return lax.dot_general(a, b, (((ca,), (cb,)), ((), ())), preferred_element_type=F32)


def normalize(values, axis=-1):
    average = jnp.mean(values, axis=axis, keepdims=True)
    centered = values - average
    inverse = lax.rsqrt(jnp.mean(centered * centered, axis=axis, keepdims=True) + epsilon)
    return (centered * inverse, inverse)


def normalize_back(gradient, normed, inverse, axis=-1):
    mean_grad = jnp.mean(gradient, axis=axis, keepdims=True)
    mean_both = jnp.mean(gradient * normed, axis=axis, keepdims=True)
    return (gradient - mean_grad - normed * mean_both) * inverse


ARBITRARY = pltpu.CompilerParams(dimension_semantics=("arbitrary",))


def prepare_body(
    me_ref, tok_ref, cot_ref, unit_ref, inv_ref, xk_ref, xs_ref, xr_ref, ck_ref, cs_ref, cr_ref, mean_ref
):
    step = pl.program_id(0)
    rows = tok_ref.shape[0]
    group, _, own, _ = xk_ref.shape
    block = 4 * own
    core = me_ref[1]

    @pl.when(step == 0)
    def _():
        values = tok_ref[...].astype(F32)
        average = jnp.mean(values, axis=-1, keepdims=True)
        centered = values - average
        inverse = lax.rsqrt(jnp.mean(centered * centered, axis=-1, keepdims=True) + epsilon)
        mean_ref[...] = jnp.broadcast_to(average, (rows, HD))
        inv_ref[...] = jnp.broadcast_to(inverse, (rows, HD))

    def slab(s, carry):
        here = pl.ds(pl.multiple_of((step * group + s) * block, HD), block)
        there = pl.ds(pl.multiple_of(s * block, HD), block)
        unit = (tok_ref[:, here].astype(F32) - mean_ref[:, :1]) * inv_ref[:, :1]
        unit_ref[:, there] = unit
        for value, refs in (
            (unit.astype(BF), (xk_ref, xs_ref, xr_ref)),
            (cot_ref[:, here], (ck_ref, cs_ref, cr_ref)),
        ):
            turned = value.T

            def place(refs, turned, c):
                for y in range(2):
                    away_y = lax.rem(me_ref[2] + y, 2)
                    at = (2 * y + c) * own
                    refs[0][s, away_y] = turned[at : at + own]
                    at = (2 * y + 1 - c) * own
                    refs[1][s, away_y] = turned[at : at + own]

            @pl.when(core == 0)
            def _():
                place(refs, turned, 0)

            @pl.when(core == 1)
            def _():
                place(refs, turned, 1)

            for c in range(2):
                refs[2][s, c] = refs[c][s].reshape(2 * own, rows).T
        return carry

    lax.fori_loop(0, group, slab, 0)


def prepare(me, tokens, cotangent, slabs, steps=4):
    rows, features = tokens.shape
    own = features // slabs // 4
    group = slabs // steps
    whole = pl.BlockSpec((rows, features), lambda i, me: (0, 0))
    turned = pl.BlockSpec((group, 2, own, rows), lambda i, me: (i, 0, 0, 0))
    plain = pl.BlockSpec((group, 2, rows, 2 * own), lambda i, me: (i, 0, 0, 0))
    turned_shape = jax.ShapeDtypeStruct((slabs, 2, own, rows), BF)
    plain_shape = jax.ShapeDtypeStruct((slabs, 2, rows, 2 * own), BF)
    return pl.pallas_call(
        prepare_body,
        grid_spec=pltpu.PrefetchScalarGridSpec(
            num_scalar_prefetch=1,
            grid=(steps,),
            in_specs=[whole, whole],
            out_specs=[
                pl.BlockSpec((rows, features // steps), lambda i, me: (0, i)),
                pl.BlockSpec((rows, HD), lambda i, me: (0, 0)),
            ]
            + [turned, turned, plain] * 2,
            scratch_shapes=[pltpu.VMEM((rows, HD), F32)],
        ),
        out_shape=[
            jax.ShapeDtypeStruct((rows, features), F32),
            jax.ShapeDtypeStruct((rows, HD), F32),
        ]
        + [turned_shape, turned_shape, plain_shape] * 2,
        compiler_params=ARBITRARY,
        name="prepare",
    )(me, tokens, cotangent)


def distance(i):
    return (i + 1) // 2 * (1 if i % 2 == 0 else -1)


def project_kv_body(me_ref, x_ref, near_ref, near_far_ref, far_ref, far_far_ref, k_ref, kl_ref, vl_ref):
    slabs = x_ref.shape[0]
    rows, width = k_ref.shape
    close = near_ref.shape[0]
    for n in range(2 * width // 256):
        cols = slice(n * 256, (n + 1) * 256)
        acc = jnp.zeros((rows, 256), F32)
        for i in range(slabs):
            slab = lax.rem(me_ref[0] + slabs + distance(i), slabs)
            if i < close:
                pieces = near_ref[i, :, cols], near_far_ref[i, :, cols]
            else:
                pieces = far_ref[i - close, :, cols], far_far_ref[i - close, :, cols]
            for c, piece in enumerate(pieces):
                acc = acc + dot(x_ref[slab, c], piece)
        for j in range(2):
            at = n * 256 + j * HD
            part = acc[:, j * HD : (j + 1) * HD]
            if at < width:
                k_ref[:, at : at + HD] = part
                kl_ref[:, at : at + HD] = normalize(part)[0].astype(BF)
            else:
                vl_ref[:, at - width : at - width + HD] = part.astype(BF)


def project_kv(me, x, near, near_far, far, far_far):
    rows, width = x.shape[2], near.shape[2] // 2
    return pl.pallas_call(
        project_kv_body,
        in_specs=[pl.BlockSpec(memory_space=pltpu.SMEM)] + [pl.BlockSpec(memory_space=pltpu.VMEM)] * 5,
        out_shape=[
            jax.ShapeDtypeStruct((rows, width), F32),
            jax.ShapeDtypeStruct((rows, width), BF),
            jax.ShapeDtypeStruct((rows, width), BF),
        ],
        name="project_kv",
    )(me, x, near, near_far, far, far_far)


def far_from(i):
    return lax.div(i + 1, 2) * (1 - 2 * lax.rem(i, 2))


def project_qo_body(me_ref, x_ref, c_ref, *refs):
    near, far, (q_ref, g_ref, acc_ref) = refs[:4], refs[4:8], refs[8:]
    slabs = x_ref.shape[0]
    width = q_ref.shape[1]
    close = near[0].shape[0]
    acc_ref[...] = jnp.zeros_like(acc_ref)

    def take(group, first):
        def step(k, carry):
            slab = lax.rem(me_ref[0] + slabs + far_from(k + first), slabs)
            for left_ref, at in ((x_ref, 0), (c_ref, width)):
                cols = slice(at, at + width)
                part = 0.0
                for c in range(2):
                    piece = jnp.concatenate([group[2 * c + y][k, :, cols] for y in range(2)], axis=0)
                    part = part + dot(left_ref[slab, c], piece)
                acc_ref[:, cols] += part
            return carry

        lax.fori_loop(0, group[0].shape[0], step, 0)

    take(near, 0)
    take(far, close)
    q_ref[...] = acc_ref[:, :width]
    g_ref[...] = acc_ref[:, width:].astype(BF)


VMEM = pl.BlockSpec(memory_space=pltpu.VMEM)
SMEM = pl.BlockSpec(memory_space=pltpu.SMEM)


def project_qo(me, x, c, near, far):
    rows, width = x.shape[2], near[0].shape[2] // 2
    return pl.pallas_call(
        project_qo_body,
        in_specs=[SMEM] + [VMEM] * 10,
        out_shape=[jax.ShapeDtypeStruct((rows, width), F32), jax.ShapeDtypeStruct((rows, width), BF)],
        scratch_shapes=[pltpu.VMEM((rows, 2 * width), F32)],
        name="project_qo",
    )(me, x, c, *near, *far)


def attend_body(q_ref, g_ref, *refs, count):
    k_refs, v_refs, (att_ref, qb_ref) = refs[:count], refs[count : 2 * count], refs[2 * count : 2 * count + 2]
    pair_refs, e_ref = refs[2 * count + 2 : 3 * count + 2], refs[3 * count + 2]
    rows = q_ref.shape[0]
    scale = HD ** (-0.5)
    q_unit, q_inv = normalize(q_ref[...])
    q = q_unit.astype(BF)
    g = g_ref[...]
    total = jnp.zeros((8, rows), F32)
    att_t = jnp.zeros((HD, rows), F32)
    at = 0
    spots = []
    for k_ref, v_ref in zip(k_refs, v_refs):
        keys = k_ref.shape[0]
        here = slice(at, at + keys)
        spots.append(here)
        at += keys
        e = jnp.exp(dot(k_ref[...], q, 1, 1) * scale)
        e_ref[here] = e
        total = total + jnp.sum(e.reshape(keys // 8, 8, rows), axis=0)
        att_t = att_t + dot(v_ref[...].T, e.astype(BF))
    total = jnp.sum(total, axis=0, keepdims=True)
    inv_total = 1.0 / total
    att = (att_t * inv_total).T.astype(BF)
    att_ref[...] = att
    delta = jnp.sum((g.astype(F32) * att.astype(F32)).T, axis=0, keepdims=True)
    dq_t = jnp.zeros((HD, rows), F32)
    for k_ref, v_ref, pair_ref, here in zip(k_refs, v_refs, pair_refs, spots):
        p = e_ref[here] * inv_total
        dp = dot(v_ref[...], g, 1, 1)
        ds = (p * ((dp - delta) * scale)).astype(BF)
        pair_ref[0] = dot(ds, q).astype(BF)
        pair_ref[1] = dot(p.astype(BF), g).astype(BF)
        dq_t = dq_t + dot(k_ref[...].T, ds)
    qb_ref[...] = normalize_back(dq_t.T, q_unit, q_inv).astype(BF)


def attend(q, g, keys, values):
    rows, width = q.shape
    sizes = [k.shape[0] for k in keys]
    row_spec = pl.BlockSpec((rows, HD), lambda h: (0, h))
    specs = [pl.BlockSpec((n, HD), lambda h: (0, h)) for n in sizes]
    return pl.pallas_call(
        lambda *refs: attend_body(*refs, count=len(sizes)),
        grid=(width // HD,),
        in_specs=[row_spec, row_spec] + specs * 2,
        out_specs=[row_spec, row_spec] + [pl.BlockSpec((2, n, HD), lambda h: (0, 0, h)) for n in sizes],
        out_shape=[jax.ShapeDtypeStruct((rows, width), BF)] * 2
        + [jax.ShapeDtypeStruct((2, n, width), BF) for n in sizes],
        scratch_shapes=[pltpu.VMEM((sum(sizes), rows), F32)],
        compiler_params=ARBITRARY,
        name="attend",
    )(q, g, *keys, *values)


def terms_of(me_ref, x_ref, c_ref, a_ref, b_ref, store):
    slabs, _, own, rows = x_ref.shape
    width = a_ref.shape[1]

    def step(k, carry):
        spots = [lax.rem(me_ref[0] + 2 * k + i, slabs) for i in range(2)]
        for left_ref, right_ref, cols in (
            (x_ref, a_ref, slice(None, width)),
            (c_ref, b_ref, slice(width, None)),
        ):
            left = jnp.concatenate([left_ref[spot].reshape(2 * own, rows) for spot in spots], axis=0)
            value = dot(left, right_ref[...])
            for i in range(2):
                for y in range(2):
                    at = (2 * i + y) * own
                    store(2 * k + i, y, cols, value[at : at + own])
        return carry

    lax.fori_loop(0, slabs // 2, step, 0)


def query_send_body(me_ref, x_ref, c_ref, a_ref, b_ref, out_ref):
    def store(r, y, cols, value):
        out_ref[y, r, :, cols] = value.astype(BF)

    terms_of(me_ref, x_ref, c_ref, a_ref, b_ref, store)


def query_keep_body(me_ref, x_ref, c_ref, a_ref, b_ref, got_ref, stay_ref, go_ref):
    def store(r, y, cols, value):
        (stay_ref, go_ref)[y][r, :, cols] = (value + got_ref[y, r, :, cols].astype(F32)).astype(BF)

    terms_of(me_ref, x_ref, c_ref, a_ref, b_ref, store)


def key_send_body(me_ref, x_ref, k_ref, own_ref, high_ref, low_ref, kb_ref, vb_ref, out_ref):
    width = k_ref.shape[1]
    total = own_ref[...].astype(F32) + high_ref[...].astype(F32) + low_ref[...].astype(F32)
    for h in range(width // HD):
        cols = slice(h * HD, (h + 1) * HD)
        unit, inv = normalize(k_ref[:, cols])
        kb_ref[:, cols] = normalize_back(total[0, :, cols], unit, inv).astype(BF)
    vb_ref[...] = total[1].astype(BF)

    def store(r, y, cols, value):
        out_ref[r, y, :, cols] = value.astype(BF)

    terms_of(me_ref, x_ref, x_ref, kb_ref, vb_ref, store)


def key_keep_body(me_ref, x_ref, a_ref, b_ref, got_ref, stay_ref, y_ref, out_ref):
    own = x_ref.shape[2]

    def store(r, y, cols, value):
        total = value + got_ref[r, y, :, cols].astype(F32)
        out_ref[r, (1 + y) * own : (2 + y) * own, cols] = total.astype(BF)

    terms_of(me_ref, x_ref, x_ref, a_ref, b_ref, store)
    for r in range(x_ref.shape[0]):
        out_ref[r, :own] = (stay_ref[r].astype(F32) + y_ref[r].astype(F32)).astype(BF)


def call(body, shapes, me, *operands):
    return pl.pallas_call(
        body, in_specs=[SMEM] + [VMEM] * len(operands), out_shape=[jax.ShapeDtypeStruct(v, BF) for v in shapes]
    )(me, *operands)


def inner_body(
    me_ref, qb_ref, kb_ref, vb_ref, near_ref, near_far_ref, far_ref, far_far_ref,
    *refs, close,
):
    step = pl.program_id(0)
    qo_near, qo_far, (unit_ref, out_ref, sum_ref, both_ref, w_ref) = refs[:4], refs[4:8], refs[8:]
    own = qo_near[0].shape[1]
    width = qb_ref.shape[1]
    away_y, away_c = me_ref[2], me_ref[1]

    def place(refs, qo_refs):
        for c, ref in enumerate(refs):
            for y in range(2):
                spot = lax.rem(away_y + y, 2), lax.rem(away_c + c, 2)
                w_ref[spot[0], spot[1], :, :width] = qo_refs[2 * c + y][0, :, :width]
                w_ref[spot[0], spot[1], :, width:] = ref[0, y * own : (y + 1) * own]

    @pl.when(step < close)
    def _():
        place((near_ref, near_far_ref), qo_near)

    @pl.when(step >= close)
    def _():
        place((far_ref, far_far_ref), qo_far)

    low = jnp.concatenate([qb_ref[...], kb_ref[...], vb_ref[...]], axis=1)
    result = dot(low, w_ref[...].reshape(4 * own, 3 * width), 1, 1)
    out_ref[0] = result.astype(BF)
    both = result * unit_ref[...]
    lanes = range(0, result.shape[1], HD)
    plain = sum(result[:, i : i + HD] for i in lanes)
    times = sum(both[:, i : i + HD] for i in lanes)

    @pl.when(step == 0)
    def _():
        sum_ref[...] = plain
        both_ref[...] = times

    @pl.when(step > 0)
    def _():
        sum_ref[...] += plain
        both_ref[...] += times


def inner(me, qb, kb, vb, near, near_far, far, far_far, qo_near, qo_far, unit):
    rows, width = qb.shape
    _, own, both = qo_near[0].shape
    close = near.shape[0]
    slabs = close + far.shape[0]

    def place(i, me):
        sign = 1 - 2 * lax.rem(i, 2)
        return lax.rem(me[0] + slabs + lax.div(i + 1, 2) * sign, slabs)

    whole = pl.BlockSpec((rows, width), lambda i, me: (0, 0))
    stat = pl.BlockSpec((rows, HD), lambda i, me: (0, 0))

    def first(rows):
        return pl.BlockSpec((1, rows, both), lambda i, me: (jnp.minimum(i, close - 1), 0, 0))

    def last(rows):
        return pl.BlockSpec((1, rows, both), lambda i, me: (jnp.maximum(i - close, 0), 0, 0))

    return pl.pallas_call(
        lambda *refs: inner_body(*refs, close=close),
        grid_spec=pltpu.PrefetchScalarGridSpec(
            num_scalar_prefetch=1,
            grid=(slabs,),
            in_specs=[whole] * 3
            + [first(2 * own)] * 2
            + [last(2 * own)] * 2
            + [first(own)] * 4
            + [last(own)] * 4
            + [pl.BlockSpec((rows, 4 * own), lambda i, me: (0, place(i, me)))],
            out_specs=[
                pl.BlockSpec((1, rows, 4 * own), lambda i, me: (place(i, me), 0, 0)),
                stat,
                stat,
            ],
            scratch_shapes=[pltpu.VMEM((2, 2, own, 3 * width), BF)],
        ),
        out_shape=[
            jax.ShapeDtypeStruct((slabs, rows, 4 * own), BF),
            jax.ShapeDtypeStruct((rows, HD), F32),
            jax.ShapeDtypeStruct((rows, HD), F32),
        ],
        compiler_params=ARBITRARY,
        name="inner",
    )(me, qb, kb, vb, near, near_far, far, far_far, *qo_near, *qo_far, unit)


def swap(value, axis):
    return lax.ppermute(value, axis, [(0, 1), (1, 0)])


def plus(a, b):
    return (a.astype(F32) + b.astype(F32)).astype(BF)


def turns():
    size = lax.axis_size("seq")
    return [(i, (i + 1) % size) for i in range(size)], [(i, (i - 1) % size) for i in range(size)]


def ring_gather(value, held=None):
    up, down = turns()
    half = value.shape[0] // 2
    rows = [value]
    high = low = value
    for step in range(len(up) // 2 - 1):
        high = lax.ppermute(high, "seq", up)
        low = lax.ppermute(low, "seq", down)
        if step == 0 and held is not None:
            high, low, held = lax.optimization_barrier((high, low, held))
        rows += [high, low]
    rows.append(lax.ppermute(high[:half], "seq", up))
    rows.append(lax.ppermute(low[half:], "seq", down))
    return rows if held is None else (rows, held)


def whole(ring):
    return ring[:-2] + [jnp.concatenate(ring[-2:], axis=0)]


def ring_reduce(part, high, low, axis):
    up, down = turns()
    size = len(up)
    half = high.shape[axis]
    for step in range(size // 2, 0, -1):
        if step == size // 2 - 1:
            mine, theirs = part(step), part(size - step)
            cut = lambda v, lo, hi: lax.slice_in_dim(v, lo, hi, axis=axis)
            high = jnp.concatenate([plus(cut(mine, 0, half), high), cut(mine, half, 2 * half)], axis=axis)
            low = jnp.concatenate([cut(theirs, 0, half), plus(cut(theirs, half, 2 * half), low)], axis=axis)
        elif step < size // 2:
            high, low = plus(part(step), high), plus(part(size - step), low)
        high = lax.ppermute(high, "seq", up)
        low = lax.ppermute(low, "seq", down)
    return high, low


def pieces_of(value):
    parts = []
    for _ in range(3):
        part = lax.reduce_precision(value, 8, 7)
        parts.append(part.astype(BF))
        value = value - part
    return parts


def layer(tokens, cotangent, qkv_weight, out_weight):
    row_count, feature_count = tokens.shape[1:]
    own, _, width = qkv_weight.shape
    slabs = lax.axis_size("seq")
    shares = lax.axis_size(("x", "yhi"))
    me = jnp.stack([lax.axis_index("seq"), lax.axis_index("core"), lax.axis_index("ylo")]).astype(jnp.int32)
    kv_weight = qkv_weight[:, 1:].reshape(own, 2 * width)
    qo_weight = jnp.concatenate([qkv_weight[:, 0], out_weight], axis=1)
    qo_ring = whole(ring_gather(qo_weight))
    kv_weight = jnp.concatenate([kv_weight, swap(kv_weight, "ylo")], axis=0)
    unit, inverse, *turned = prepare(me, tokens[0], cotangent[0], slabs)
    x_keep, x_send, x_r, c_keep, c_send, c_r = turned
    ring, x_r = ring_gather(kv_weight, x_r)
    ring = whole(ring)
    near, far = jnp.stack(ring[:5]), jnp.stack(ring[5:])
    near_far, far_far = swap(near, "core"), swap(far, "core")
    key, key_low, value_low = project_kv(me, x_r, near, near_far, far, far_far)

    def spread(mine):
        across = swap(mine, "ylo")
        return mine, across, swap(mine, "core"), swap(across, "core")

    qo_near, qo_far = spread(jnp.stack(qo_ring[:5])), spread(jnp.stack(qo_ring[5:]))
    keys, values = ring_gather(key_low), ring_gather(value_low)
    query, grad_rows = project_qo(me, x_r, c_r, qo_near, qo_far)
    attended, query_back, *pairs = attend(query, grad_rows, keys, values)
    where = {distance(i) % slabs: pairs[i] for i in range(slabs - 1)}
    high, low = ring_reduce(lambda r: where[r], pairs[-2], pairs[-1], 1)
    both = 2 * width
    got = call(query_send_body, [(2, slabs, own, both)], me, x_send, c_send, query_back, attended)[0]
    got = swap(got, "core")
    stay, go = call(
        query_keep_body, [(slabs, own, both)] * 2, me, x_keep, c_keep, query_back, attended, got
    )
    from_y = swap(go, "ylo")
    key, from_y = lax.optimization_barrier((key, from_y))
    key_grad, value_grad, send = call(
        key_send_body,
        [(row_count, width)] * 2 + [(slabs, 2, own, both)],
        me, x_send, key, where[0], high, low,
    )
    merged = call(
        key_keep_body,
        [(slabs, 3 * own, both)],
        me, x_keep, key_grad, value_grad, swap(send, "core"), stay, from_y,
    )[0]
    merged, key_grad = lax.optimization_barrier((merged, key_grad))
    half = 3 * own // 2
    far_part = merged[slabs // 2]
    high, low = ring_reduce(lambda r: merged[r], far_part[:half], far_part[half:], 0)
    share, plain, both = inner(
        me, query_back, key_grad, value_grad, near, near_far, far, far_far, qo_near, qo_far, unit
    )
    stats = jnp.stack(pieces_of(jnp.sum(plain, axis=1)) + pieces_of(jnp.sum(both, axis=1)))
    stats = stats.reshape(-1, share.shape[2])
    stats = jnp.pad(stats, ((0, 16 - stats.shape[0]), (0, 0)))
    load = jnp.concatenate([share, jnp.broadcast_to(stats, (shares, *stats.shape))], axis=1)
    load = lax.all_to_all(load, ("x", "yhi"), 0, 0, tiled=True)
    load, high, low = lax.optimization_barrier((load, high, low))
    summed = merged[0].astype(F32) + high.astype(F32) + low.astype(F32)
    query_out = summed[:own]
    key_value_grad = summed[own : 2 * own] + swap(summed[2 * own :].astype(BF), "ylo").astype(F32)
    load = load.astype(F32)
    load = jnp.sum(load, axis=0)
    own_share = load[:row_count]
    totals = load[row_count:].reshape(-1)[: 6 * row_count].reshape(2, 3, row_count)
    totals = jnp.sum(totals, axis=1)[:, :, None] / feature_count
    offset = lax.axis_index(("x", "yhi")) * share.shape[2]
    unit_own = lax.dynamic_slice_in_dim(unit, offset, share.shape[2], 1)
    branch = (own_share - totals[0] - unit_own * totals[1]) * inverse[:, :1]
    qkv_grad = jnp.stack(
        [query_out[:, :width], key_value_grad[:, :width], key_value_grad[:, width:]], axis=1
    )
    return (qkv_grad, query_out[:, width:], branch.astype(BF)[None])


def solution(mesh):
    split = jax.sharding.Mesh(
        mesh.devices.reshape(mesh.shape["seq"], mesh.shape["tensor"] // 2, 2, 2, 2),
        ("seq", "x", "yhi", "ylo", "core"),
    )
    blocks = ("seq", "ylo", "core")
    heads = ("x", "yhi")
    return jax.shard_map(
        layer,
        mesh=split,
        in_specs=(
            P(("ylo", "core"), "seq", None),
            P(("ylo", "core"), "seq", None),
            P(blocks, None, heads),
            P(blocks, heads),
        ),
        out_specs=(
            P(blocks, None, heads),
            P(blocks, heads),
            P(("ylo", "core"), "seq", heads),
        ),
        check_vma=False,
    )
```

```python
import jax
import jax.numpy as jnp
from jax import lax
from jax.experimental import pallas as pl
from jax.experimental.pallas import tpu as pltpu
from jax.sharding import PartitionSpec as P

HD = 128
epsilon = 1e-06
BF = jnp.bfloat16
F32 = jnp.float32


def dot(a, b, ca=1, cb=0):
    return lax.dot_general(a, b, (((ca,), (cb,)), ((), ())), preferred_element_type=F32)


def normalize(values, axis=-1):
    average = jnp.mean(values, axis=axis, keepdims=True)
    centered = values - average
    inverse = lax.rsqrt(jnp.mean(centered * centered, axis=axis, keepdims=True) + epsilon)
    return (centered * inverse, inverse)


def normalize_back(gradient, normed, inverse, axis=-1):
    mean_grad = jnp.mean(gradient, axis=axis, keepdims=True)
    mean_both = jnp.mean(gradient * normed, axis=axis, keepdims=True)
    return (gradient - mean_grad - normed * mean_both) * inverse


ARBITRARY = pltpu.CompilerParams(dimension_semantics=("arbitrary",))


def prepare_body(
    me_ref, tok_ref, cot_ref, unit_ref, inv_ref, xk_ref, xs_ref, xr_ref, ck_ref, cs_ref, cr_ref, mean_ref
):
    step = pl.program_id(0)
    rows = tok_ref.shape[0]
    group, _, own, _ = xk_ref.shape
    block = 4 * own
    core = me_ref[1]

    @pl.when(step == 0)
    def _():
        values = tok_ref[...].astype(F32)
        average = jnp.mean(values, axis=-1, keepdims=True)
        centered = values - average
        inverse = lax.rsqrt(jnp.mean(centered * centered, axis=-1, keepdims=True) + epsilon)
        mean_ref[...] = jnp.broadcast_to(average, (rows, HD))
        inv_ref[...] = jnp.broadcast_to(inverse, (rows, HD))

    def slab(s, carry):
        here = pl.ds(pl.multiple_of((step * group + s) * block, HD), block)
        there = pl.ds(pl.multiple_of(s * block, HD), block)
        unit = (tok_ref[:, here].astype(F32) - mean_ref[:, :1]) * inv_ref[:, :1]
        unit_ref[:, there] = unit
        for value, refs in (
            (unit.astype(BF), (xk_ref, xs_ref, xr_ref)),
            (cot_ref[:, here], (ck_ref, cs_ref, cr_ref)),
        ):
            turned = value.T

            def place(refs, turned, c):
                for y in range(2):
                    away_y = lax.rem(me_ref[2] + y, 2)
                    at = (2 * y + c) * own
                    refs[0][s, away_y] = turned[at : at + own]
                    at = (2 * y + 1 - c) * own
                    refs[1][s, away_y] = turned[at : at + own]

            @pl.when(core == 0)
            def _():
                place(refs, turned, 0)

            @pl.when(core == 1)
            def _():
                place(refs, turned, 1)

            for c in range(2):
                refs[2][s, c] = refs[c][s].reshape(2 * own, rows).T
        return carry

    lax.fori_loop(0, group, slab, 0)


def prepare(me, tokens, cotangent, slabs, steps=4):
    rows, features = tokens.shape
    own = features // slabs // 4
    group = slabs // steps
    whole = pl.BlockSpec((rows, features), lambda i, me: (0, 0))
    turned = pl.BlockSpec((group, 2, own, rows), lambda i, me: (i, 0, 0, 0))
    plain = pl.BlockSpec((group, 2, rows, 2 * own), lambda i, me: (i, 0, 0, 0))
    turned_shape = jax.ShapeDtypeStruct((slabs, 2, own, rows), BF)
    plain_shape = jax.ShapeDtypeStruct((slabs, 2, rows, 2 * own), BF)
    return pl.pallas_call(
        prepare_body,
        grid_spec=pltpu.PrefetchScalarGridSpec(
            num_scalar_prefetch=1,
            grid=(steps,),
            in_specs=[whole, whole],
            out_specs=[
                pl.BlockSpec((rows, features // steps), lambda i, me: (0, i)),
                pl.BlockSpec((rows, HD), lambda i, me: (0, 0)),
            ]
            + [turned, turned, plain] * 2,
            scratch_shapes=[pltpu.VMEM((rows, HD), F32)],
        ),
        out_shape=[
            jax.ShapeDtypeStruct((rows, features), F32),
            jax.ShapeDtypeStruct((rows, HD), F32),
        ]
        + [turned_shape, turned_shape, plain_shape] * 2,
        compiler_params=ARBITRARY,
        name="prepare",
    )(me, tokens, cotangent)


def distance(i):
    return (i + 1) // 2 * (1 if i % 2 == 0 else -1)


def far_from(i):
    return lax.div(i + 1, 2) * (1 - 2 * lax.rem(i, 2))


def project_kv_body(
    me_ref, x_ref, near_ref, near_far_ref, far_ref, far_far_ref, k_ref, kl_ref, vl_ref, acc_ref
):
    slabs = x_ref.shape[0]
    width = k_ref.shape[1]
    close = near_ref.shape[0]
    acc_ref[...] = jnp.zeros_like(acc_ref)

    def take(mine_ref, theirs_ref, first):
        def step(k, carry):
            slab = lax.rem(me_ref[0] + slabs + far_from(k + first), slabs)
            acc_ref[...] += dot(x_ref[slab, 0], mine_ref[k]) + dot(x_ref[slab, 1], theirs_ref[k])
            return carry

        lax.fori_loop(0, mine_ref.shape[0], step, 0)

    take(near_ref, near_far_ref, 0)
    take(far_ref, far_far_ref, close)
    k_ref[...] = acc_ref[:, :width]
    for at in range(0, width, HD):
        kl_ref[:, at : at + HD] = normalize(acc_ref[:, at : at + HD])[0].astype(BF)
    vl_ref[...] = acc_ref[:, width:].astype(BF)


def project_kv(me, x, near, near_far, far, far_far):
    rows, width = x.shape[2], near.shape[2] // 2
    return pl.pallas_call(
        project_kv_body,
        in_specs=[pl.BlockSpec(memory_space=pltpu.SMEM)] + [pl.BlockSpec(memory_space=pltpu.VMEM)] * 5,
        out_shape=[
            jax.ShapeDtypeStruct((rows, width), F32),
            jax.ShapeDtypeStruct((rows, width), BF),
            jax.ShapeDtypeStruct((rows, width), BF),
        ],
        scratch_shapes=[pltpu.VMEM((rows, 2 * width), F32)],
        name="project_kv",
    )(me, x, near, near_far, far, far_far)


def project_qo_body(x_ref, c_ref, b_ref, by_ref, bc_ref, byc_ref, q_ref, g_ref, acc_ref):
    slabs = x_ref.shape[0]
    width = q_ref.shape[1]
    acc_ref[...] = jnp.zeros_like(acc_ref)

    def step(k, carry):
        for left_ref, at in ((x_ref, 0), (c_ref, width)):
            cols = slice(at, at + width)
            part = 0.0
            for c, (first, second) in enumerate(((b_ref, by_ref), (bc_ref, byc_ref))):
                piece = jnp.concatenate([first[k, :, cols], second[k, :, cols]], axis=0)
                part = part + dot(left_ref[k, c], piece)
            acc_ref[:, cols] += part
        return carry

    lax.fori_loop(0, slabs, step, 0)
    q_ref[...] = acc_ref[:, :width]
    g_ref[...] = acc_ref[:, width:].astype(BF)


VMEM = pl.BlockSpec(memory_space=pltpu.VMEM)
SMEM = pl.BlockSpec(memory_space=pltpu.SMEM)


def project_qo(x, c, *pieces):
    rows, width = x.shape[2], pieces[0].shape[2] // 2
    return pl.pallas_call(
        project_qo_body,
        in_specs=[VMEM] * 6,
        out_shape=[jax.ShapeDtypeStruct((rows, width), F32), jax.ShapeDtypeStruct((rows, width), BF)],
        scratch_shapes=[pltpu.VMEM((rows, 2 * width), F32)],
        name="project_qo",
    )(x, c, *pieces)


def attend_body(me_ref, q_ref, g_ref, *refs, count):
    k_refs, v_refs = refs[:count], refs[count : 2 * count]
    att_ref, qb_ref, pair_ref, e_ref = refs[2 * count :]
    slabs = pair_ref.shape[0]
    rows = q_ref.shape[0]
    scale = HD ** (-0.5)
    q_unit, q_inv = normalize(q_ref[...])
    q = q_unit.astype(BF)
    g = g_ref[...]
    total = jnp.zeros((8, rows), F32)
    att_t = jnp.zeros((HD, rows), F32)
    at = 0
    spots = []
    for k_ref, v_ref in zip(k_refs, v_refs):
        keys = k_ref.shape[0]
        here = slice(at, at + keys)
        spots.append(here)
        at += keys
        e = jnp.exp(dot(k_ref[...], q, 1, 1) * scale)
        e_ref[here] = e
        total = total + jnp.sum(e.reshape(keys // 8, 8, rows), axis=0)
        att_t = att_t + dot(v_ref[...].T, e.astype(BF))
    total = jnp.sum(total, axis=0, keepdims=True)
    inv_total = 1.0 / total
    att = (att_t * inv_total).T.astype(BF)
    att_ref[...] = att
    delta = jnp.sum((g.astype(F32) * att.astype(F32)).T, axis=0, keepdims=True)
    dq_t = jnp.zeros((HD, rows), F32)
    for i, (k_ref, v_ref, here) in enumerate(zip(k_refs, v_refs, spots)):
        p = e_ref[here] * inv_total
        dp = dot(v_ref[...], g, 1, 1)
        ds = (p * ((dp - delta) * scale)).astype(BF)
        slab = lax.rem(me_ref[0] + slabs + distance(i), slabs)
        pair_ref[slab, 0] = dot(ds, q).astype(BF)
        pair_ref[slab, 1] = dot(p.astype(BF), g).astype(BF)
        dq_t = dq_t + dot(k_ref[...].T, ds)
    qb_ref[...] = normalize_back(dq_t.T, q_unit, q_inv).astype(BF)


def attend(me, q, g, keys, values):
    rows, width = q.shape
    sizes = [k.shape[0] for k in keys]
    shape = (sum(sizes) // rows, 2, rows, width)
    row_spec = pl.BlockSpec((rows, HD), lambda h, me: (0, h))
    specs = [pl.BlockSpec((n, HD), lambda h, me: (0, h)) for n in sizes]
    return pl.pallas_call(
        lambda *refs: attend_body(*refs, count=len(sizes)),
        grid_spec=pltpu.PrefetchScalarGridSpec(
            num_scalar_prefetch=1,
            grid=(width // HD,),
            in_specs=[row_spec, row_spec] + specs * 2,
            out_specs=[
                row_spec,
                row_spec,
                pl.BlockSpec((*shape[:3], HD), lambda h, me: (0, 0, 0, h)),
            ],
            scratch_shapes=[pltpu.VMEM((sum(sizes), rows), F32)],
        ),
        out_shape=[
            jax.ShapeDtypeStruct((rows, width), BF),
            jax.ShapeDtypeStruct((rows, width), BF),
            jax.ShapeDtypeStruct(shape, BF),
        ],
        compiler_params=ARBITRARY,
        name="attend",
    )(me, q, g, *keys, *values)


def terms_of(x_ref, c_ref, a_ref, b_ref, store):
    slabs, _, own, rows = x_ref.shape
    width = a_ref.shape[1]

    def step(k, carry):
        spots = [2 * k + i for i in range(2)]
        for left_ref, right_ref, cols in (
            (x_ref, a_ref, slice(None, width)),
            (c_ref, b_ref, slice(width, None)),
        ):
            left = jnp.concatenate([left_ref[spot].reshape(2 * own, rows) for spot in spots], axis=0)
            value = dot(left, right_ref[...])
            for i in range(2):
                for y in range(2):
                    at = (2 * i + y) * own
                    store(2 * k + i, y, cols, value[at : at + own])
        return carry

    lax.fori_loop(0, slabs // 2, step, 0)


def query_send_body(x_ref, c_ref, a_ref, b_ref, out_ref):
    def store(r, y, cols, value):
        out_ref[y, r, :, cols] = value.astype(BF)

    terms_of(x_ref, c_ref, a_ref, b_ref, store)


def query_keep_body(x_ref, c_ref, a_ref, b_ref, got_ref, stay_ref, go_ref):
    def store(r, y, cols, value):
        (stay_ref, go_ref)[y][r, :, cols] = (value + got_ref[y, r, :, cols].astype(F32)).astype(BF)

    terms_of(x_ref, c_ref, a_ref, b_ref, store)


def key_send_body(x_ref, k_ref, sum_ref, kb_ref, vb_ref, out_ref):
    width = k_ref.shape[1]
    rows = k_ref.shape[0]
    for h in range(width // HD):
        cols = slice(h * HD, (h + 1) * HD)
        unit, inv = normalize(k_ref[:, cols])
        kb_ref[:, cols] = normalize_back(sum_ref[:rows, cols].astype(F32), unit, inv).astype(BF)
    vb_ref[...] = sum_ref[rows:]

    def store(r, y, cols, value):
        out_ref[r, y, :, cols] = value.astype(BF)

    terms_of(x_ref, x_ref, kb_ref, vb_ref, store)


def key_keep_body(x_ref, a_ref, b_ref, got_ref, stay_ref, y_ref, out_ref):
    own = x_ref.shape[2]

    def store(r, y, cols, value):
        total = value + got_ref[r, y, :, cols].astype(F32)
        out_ref[r, (1 + y) * own : (2 + y) * own, cols] = total.astype(BF)

    terms_of(x_ref, x_ref, a_ref, b_ref, store)
    for r in range(x_ref.shape[0]):
        out_ref[r, :own] = (stay_ref[r].astype(F32) + y_ref[r].astype(F32)).astype(BF)


def call(body, shapes, *operands):
    return pl.pallas_call(
        body,
        in_specs=[VMEM] * len(operands),
        out_shape=[jax.ShapeDtypeStruct(v, BF) for v in shapes],
    )(*operands)


def inner_body(
    me_ref, qb_ref, kb_ref, vb_ref, near_ref, near_far_ref, far_ref, far_far_ref,
    *refs, close,
):
    step = pl.program_id(0)
    qo_refs, (unit_ref, out_ref, sum_ref, both_ref, w_ref) = refs[:4], refs[4:]
    own = qo_refs[0].shape[1]
    width = qb_ref.shape[1]
    away_y, away_c = me_ref[2], me_ref[1]

    def place(refs):
        for c, ref in enumerate(refs):
            for y in range(2):
                spot = lax.rem(away_y + y, 2), lax.rem(away_c + c, 2)
                w_ref[spot[0], spot[1], :, :width] = qo_refs[2 * c + y][0, :, :width]
                w_ref[spot[0], spot[1], :, width:] = ref[0, y * own : (y + 1) * own]

    @pl.when(step < close)
    def _():
        place((near_ref, near_far_ref))

    @pl.when(step >= close)
    def _():
        place((far_ref, far_far_ref))

    low = jnp.concatenate([qb_ref[...], kb_ref[...], vb_ref[...]], axis=1)
    result = dot(low, w_ref[...].reshape(4 * own, 3 * width), 1, 1)
    out_ref[0] = result.astype(BF)
    both = result * unit_ref[...]
    lanes = range(0, result.shape[1], HD)
    plain = sum(result[:, i : i + HD] for i in lanes)
    times = sum(both[:, i : i + HD] for i in lanes)

    @pl.when(step == 0)
    def _():
        sum_ref[...] = plain
        both_ref[...] = times

    @pl.when(step > 0)
    def _():
        sum_ref[...] += plain
        both_ref[...] += times


def inner(me, qb, kb, vb, near, near_far, far, far_far, pieces, unit):
    rows, width = qb.shape
    _, own, both = pieces[0].shape
    close = near.shape[0]
    slabs = close + far.shape[0]

    def place(i, me):
        sign = 1 - 2 * lax.rem(i, 2)
        return lax.rem(me[0] + slabs + lax.div(i + 1, 2) * sign, slabs)

    whole = pl.BlockSpec((rows, width), lambda i, me: (0, 0))
    stat = pl.BlockSpec((rows, HD), lambda i, me: (0, 0))

    def first(rows):
        return pl.BlockSpec((1, rows, both), lambda i, me: (jnp.minimum(i, close - 1), 0, 0))

    def last(rows):
        return pl.BlockSpec((1, rows, both), lambda i, me: (jnp.maximum(i - close, 0), 0, 0))

    return pl.pallas_call(
        lambda *refs: inner_body(*refs, close=close),
        grid_spec=pltpu.PrefetchScalarGridSpec(
            num_scalar_prefetch=1,
            grid=(slabs,),
            in_specs=[whole] * 3
            + [first(2 * own)] * 2
            + [last(2 * own)] * 2
            + [pl.BlockSpec((1, own, both), lambda i, me: (place(i, me), 0, 0))] * 4
            + [pl.BlockSpec((rows, 4 * own), lambda i, me: (0, place(i, me)))],
            out_specs=[
                pl.BlockSpec((1, rows, 4 * own), lambda i, me: (place(i, me), 0, 0)),
                stat,
                stat,
            ],
            scratch_shapes=[pltpu.VMEM((2, 2, own, 3 * width), BF)],
        ),
        out_shape=[
            jax.ShapeDtypeStruct((slabs, rows, 4 * own), BF),
            jax.ShapeDtypeStruct((rows, HD), F32),
            jax.ShapeDtypeStruct((rows, HD), F32),
        ],
        compiler_params=ARBITRARY,
        name="inner",
    )(me, qb, kb, vb, near, near_far, far, far_far, *pieces, unit)


def swap(value, axis):
    return lax.ppermute(value, axis, [(0, 1), (1, 0)])


def turns():
    size = lax.axis_size("seq")
    return [(i, (i + 1) % size) for i in range(size)], [(i, (i - 1) % size) for i in range(size)]


def ring_gather(value, held=None, last=None):
    up, down = turns()
    half = value.shape[0] // 2
    rows = [value]
    high = low = value
    for step in range(len(up) // 2 - 1):
        high = lax.ppermute(high, "seq", up)
        low = lax.ppermute(low, "seq", down)
        if step == 0 and held is not None:
            high, low, held = lax.optimization_barrier((high, low, held))
        rows += [high, low]
    if last is None:
        rows.append(lax.ppermute(high[:half], "seq", up))
        rows.append(lax.ppermute(low[half:], "seq", down))
    else:
        rows.append(lax.ppermute(high, "seq", up) if last else lax.ppermute(low, "seq", down))
    return rows if held is None else (rows, held)


def whole(ring):
    return ring[:-2] + [jnp.concatenate(ring[-2:], axis=0)]


def pieces_of(value):
    parts = []
    for _ in range(3):
        part = lax.reduce_precision(value, 8, 7)
        parts.append(part.astype(BF))
        value = value - part
    return parts


def layer(tokens, cotangent, qkv_weight, out_weight):
    row_count, feature_count = tokens.shape[1:]
    own, _, width = qkv_weight.shape
    slabs = lax.axis_size("seq")
    shares = lax.axis_size(("x", "yhi"))
    me = jnp.stack([lax.axis_index("seq"), lax.axis_index("core"), lax.axis_index("ylo")]).astype(jnp.int32)
    kv_weight = qkv_weight[:, 1:].reshape(own, 2 * width)
    qo_weight = jnp.concatenate([qkv_weight[:, 0], out_weight], axis=1)
    qo_mine = lax.all_gather(qo_weight, "seq")
    kv_weight = jnp.concatenate([kv_weight, swap(kv_weight, "ylo")], axis=0)
    unit, inverse, *turned = prepare(me, tokens[0], cotangent[0], slabs)
    x_keep, x_send, x_r, c_keep, c_send, c_r = turned
    ring, x_r = ring_gather(kv_weight, x_r)
    ring = whole(ring)
    near, far = jnp.stack(ring[:5]), jnp.stack(ring[5:])
    near_far, far_far = swap(near, "core"), swap(far, "core")
    qo_y = swap(qo_mine, "ylo")
    key, key_low, value_low = project_kv(me, x_r, near, near_far, far, far_far)
    keys = ring_gather(key_low, last=True)
    values = ring_gather(value_low, last=False)
    qo_pieces = (qo_mine, qo_y, swap(qo_mine, "core"), swap(qo_y, "core"))
    query, grad_rows = project_qo(x_r, c_r, *qo_pieces)
    attended, query_back, pair = attend(me, query, grad_rows, keys, values)
    pair = lax.psum_scatter(
        pair.reshape(slabs * 2 * row_count, width), "seq", scatter_dimension=0, tiled=True
    )
    both = 2 * width
    got = swap(call(query_send_body, [(2, slabs, own, both)], x_send, c_send, query_back, attended)[0], "core")
    stay, go = call(query_keep_body, [(slabs, own, both)] * 2, x_keep, c_keep, query_back, attended, got)
    from_y = swap(go, "ylo")
    key, from_y = lax.optimization_barrier((key, from_y))
    key_grad, value_grad, send = call(
        key_send_body, [(row_count, width)] * 2 + [(slabs, 2, own, both)], x_send, key, pair
    )
    merged = call(
        key_keep_body,
        [(slabs, 3 * own, both)],
        x_keep, key_grad, value_grad, swap(send, "core"), stay, from_y,
    )[0]
    merged, key_grad = lax.optimization_barrier((merged, key_grad))
    merged = lax.psum_scatter(
        merged.reshape(slabs * 3 * own, both), "seq", scatter_dimension=0, tiled=True
    )
    query_out = merged[:own].astype(F32)
    key_value_grad = merged[own : 2 * own].astype(F32) + swap(merged[2 * own :], "ylo").astype(F32)
    share, plain, both = inner(
        me, query_back, key_grad, value_grad, near, near_far, far, far_far, qo_pieces, unit
    )
    stats = jnp.stack(pieces_of(jnp.sum(plain, axis=1)) + pieces_of(jnp.sum(both, axis=1)))
    stats = stats.reshape(-1, share.shape[2])
    stats = jnp.pad(stats, ((0, 16 - stats.shape[0]), (0, 0)))
    load = jnp.concatenate([share, jnp.broadcast_to(stats, (shares, *stats.shape))], axis=1)
    load = lax.all_to_all(load, ("x", "yhi"), 0, 0, tiled=True)
    load = load.astype(F32)
    load = jnp.sum(load, axis=0)
    own_share = load[:row_count]
    totals = load[row_count:].reshape(-1)[: 6 * row_count].reshape(2, 3, row_count)
    totals = jnp.sum(totals, axis=1)[:, :, None] / feature_count
    offset = lax.axis_index(("x", "yhi")) * share.shape[2]
    unit_own = lax.dynamic_slice_in_dim(unit, offset, share.shape[2], 1)
    branch = (own_share - totals[0] - unit_own * totals[1]) * inverse[:, :1]
    qkv_grad = jnp.stack(
        [query_out[:, :width], key_value_grad[:, :width], key_value_grad[:, width:]], axis=1
    )
    return (qkv_grad, query_out[:, width:], branch.astype(BF)[None])


def solution(mesh):
    split = jax.sharding.Mesh(
        mesh.devices.reshape(mesh.shape["seq"], mesh.shape["tensor"] // 2, 2, 2, 2),
        ("seq", "x", "yhi", "ylo", "core"),
    )
    blocks = ("seq", "ylo", "core")
    heads = ("x", "yhi")
    return jax.shard_map(
        layer,
        mesh=split,
        in_specs=(
            P(("ylo", "core"), "seq", None),
            P(("ylo", "core"), "seq", None),
            P(blocks, None, heads),
            P(blocks, heads),
        ),
        out_specs=(
            P(blocks, None, heads),
            P(blocks, heads),
            P(("ylo", "core"), "seq", heads),
        ),
        check_vma=False,
    )
```

```python
import jax
import jax.numpy as jnp
from jax import lax
from jax.experimental import pallas as pl
from jax.experimental.pallas import tpu as pltpu
from jax.sharding import PartitionSpec as P

HD = 128
epsilon = 1e-06
BF = jnp.bfloat16
F32 = jnp.float32


def dot(a, b, ca=1, cb=0):
    return lax.dot_general(a, b, (((ca,), (cb,)), ((), ())), preferred_element_type=F32)


def normalize(values, axis=-1):
    average = jnp.mean(values, axis=axis, keepdims=True)
    centered = values - average
    inverse = lax.rsqrt(jnp.mean(centered * centered, axis=axis, keepdims=True) + epsilon)
    return (centered * inverse, inverse)


def normalize_back(gradient, normed, inverse, axis=-1):
    mean_grad = jnp.mean(gradient, axis=axis, keepdims=True)
    mean_both = jnp.mean(gradient * normed, axis=axis, keepdims=True)
    return (gradient - mean_grad - normed * mean_both) * inverse


VMEM = pl.BlockSpec(memory_space=pltpu.VMEM)
SMEM = pl.BlockSpec(memory_space=pltpu.SMEM)
ARBITRARY = pltpu.CompilerParams(dimension_semantics=("arbitrary",))


def arrange(me_ref, value, s, keep_ref, send_ref, plain_ref):
    own, rows = keep_ref.shape[2:]
    turned = value.T

    def place(c):
        for y in range(2):
            away_y = lax.rem(me_ref[2] + y, 2)
            for ref, at in ((keep_ref, 2 * y + c), (send_ref, 2 * y + 1 - c)):
                ref[s, away_y] = turned[at * own : (at + 1) * own]

    @pl.when(me_ref[1] == 0)
    def _():
        place(0)

    @pl.when(me_ref[1] == 1)
    def _():
        place(1)

    for c, ref in enumerate((keep_ref, send_ref)):
        plain_ref[s, c] = ref[s].reshape(2 * own, rows).T


def tokens_body(me_ref, tok_ref, unit_ref, inv_ref, keep_ref, send_ref, plain_ref, mean_ref):
    rows, features = tok_ref.shape
    slabs = keep_ref.shape[0]
    block = features // slabs
    values = tok_ref[...].astype(F32)
    average = jnp.mean(values, axis=-1, keepdims=True)
    centered = values - average
    inverse = lax.rsqrt(jnp.mean(centered * centered, axis=-1, keepdims=True) + epsilon)
    mean_ref[...] = jnp.broadcast_to(average, (rows, HD))
    inv_ref[...] = jnp.broadcast_to(inverse, (rows, HD))

    def slab(s, carry):
        here = pl.ds(pl.multiple_of(s * block, HD), block)
        unit = (tok_ref[:, here].astype(F32) - mean_ref[:, :1]) * inv_ref[:, :1]
        unit_ref[:, here] = unit
        arrange(me_ref, unit.astype(BF), s, keep_ref, send_ref, plain_ref)
        return carry

    lax.fori_loop(0, slabs, slab, 0)


def cotangent_body(me_ref, cot_ref, keep_ref, send_ref, plain_ref):
    slabs = keep_ref.shape[0]
    block = cot_ref.shape[1] // slabs

    def slab(s, carry):
        here = pl.ds(pl.multiple_of(s * block, HD), block)
        arrange(me_ref, cot_ref[:, here], s, keep_ref, send_ref, plain_ref)
        return carry

    lax.fori_loop(0, slabs, slab, 0)


def prepare(me, values, slabs, tokens):
    rows, features = values.shape
    own = features // slabs // 4
    turned = jax.ShapeDtypeStruct((slabs, 2, own, rows), BF)
    extra = [
        jax.ShapeDtypeStruct((rows, features), F32),
        jax.ShapeDtypeStruct((rows, HD), F32),
    ]
    return pl.pallas_call(
        tokens_body if tokens else cotangent_body,
        in_specs=[SMEM, VMEM],
        out_shape=(extra if tokens else [])
        + [turned, turned, jax.ShapeDtypeStruct((slabs, 2, rows, 2 * own), BF)],
        scratch_shapes=[pltpu.VMEM((rows, HD), F32)] if tokens else [],
        name="prepare_tokens" if tokens else "prepare_cotangent",
    )(me, values)


def distance(i):
    return (i + 1) // 2 * (1 if i % 2 == 0 else -1)


def project_kv_body(me_ref, x_ref, near_ref, near_far_ref, far_ref, far_far_ref, k_ref, kv_ref):
    slabs = x_ref.shape[0]
    rows, width = k_ref.shape
    close = near_ref.shape[0]
    for n in range(2 * width // 256):
        cols = slice(n * 256, (n + 1) * 256)
        acc = jnp.zeros((rows, 256), F32)
        for i in range(slabs):
            slab = lax.rem(me_ref[0] + slabs + distance(i), slabs)
            if i < close:
                pieces = near_ref[i, :, cols], near_far_ref[i, :, cols]
            else:
                pieces = far_ref[i - close, :, cols], far_far_ref[i - close, :, cols]
            for c, piece in enumerate(pieces):
                acc = acc + dot(x_ref[slab, c], piece)
        for j in range(2):
            at = n * 256 + j * HD
            part = acc[:, j * HD : (j + 1) * HD]
            if at < width:
                k_ref[:, at : at + HD] = part
                kv_ref[:rows, at : at + HD] = normalize(part)[0].astype(BF)
            else:
                kv_ref[rows:, at - width : at - width + HD] = part.astype(BF)


def project_kv(me, x, near, near_far, far, far_far):
    rows, width = x.shape[2], near.shape[2] // 2
    return pl.pallas_call(
        project_kv_body,
        in_specs=[pl.BlockSpec(memory_space=pltpu.SMEM)] + [pl.BlockSpec(memory_space=pltpu.VMEM)] * 5,
        out_shape=[
            jax.ShapeDtypeStruct((rows, width), F32),
            jax.ShapeDtypeStruct((2 * rows, width), BF),
        ],
        name="project_kv",
    )(me, x, near, near_far, far, far_far)


def project_qo_body(x_ref, c_ref, b_ref, by_ref, bc_ref, byc_ref, q_ref, g_ref):
    slabs = x_ref.shape[0]
    rows, width = q_ref.shape
    for left_ref, out_ref, first in ((x_ref, q_ref, 0), (c_ref, g_ref, width)):
        for at, size in ((0, 256), (256, 128)):
            cols = slice(first + at, first + at + size)
            acc = jnp.zeros((rows, size), F32)
            for k in range(slabs):
                for c, (one, two) in enumerate(((b_ref, by_ref), (bc_ref, byc_ref))):
                    piece = jnp.concatenate([one[k, :, cols], two[k, :, cols]], axis=0)
                    acc = acc + dot(left_ref[k, c], piece)
            out_ref[:, at : at + size] = acc.astype(out_ref.dtype)


def project_qo(x, c, *pieces):
    rows, width = x.shape[2], pieces[0].shape[2] // 2
    return pl.pallas_call(
        project_qo_body,
        in_specs=[VMEM] * 6,
        out_shape=[jax.ShapeDtypeStruct((rows, width), F32), jax.ShapeDtypeStruct((rows, width), BF)],
        name="project_qo",
    )(x, c, *pieces)


def attend_body(me_ref, q_ref, g_ref, *refs):
    pieces = refs[:-4]
    att_ref, qb_ref, pair_ref, e_ref = refs[-4:]
    slabs = pair_ref.shape[0]
    rows = q_ref.shape[0]
    k_refs = [ref.at[:rows] for ref in pieces[:-2]] + [pieces[-2]]
    v_refs = [ref.at[rows:] for ref in pieces[:-2]] + [pieces[-1]]
    scale = HD ** (-0.5)
    q_unit, q_inv = normalize(q_ref[...])
    q = q_unit.astype(BF)
    g = g_ref[...]
    total = jnp.zeros((8, rows), F32)
    att_t = jnp.zeros((HD, rows), F32)
    at = 0
    spots = []
    for k_ref, v_ref in zip(k_refs, v_refs):
        keys = k_ref.shape[0]
        here = slice(at, at + keys)
        spots.append(here)
        at += keys
        e = jnp.exp(dot(k_ref[...], q, 1, 1) * scale)
        e_ref[here] = e
        total = total + jnp.sum(e.reshape(keys // 8, 8, rows), axis=0)
        att_t = att_t + dot(v_ref[...].T, e.astype(BF))
    total = jnp.sum(total, axis=0, keepdims=True)
    inv_total = 1.0 / total
    att = (att_t * inv_total).T.astype(BF)
    att_ref[...] = att
    delta = jnp.sum((g.astype(F32) * att.astype(F32)).T, axis=0, keepdims=True)
    dq_t = jnp.zeros((HD, rows), F32)
    for i, (k_ref, v_ref, here) in enumerate(zip(k_refs, v_refs, spots)):
        p = e_ref[here] * inv_total
        dp = dot(v_ref[...], g, 1, 1)
        ds = (p * ((dp - delta) * scale)).astype(BF)
        slab = lax.rem(me_ref[0] + slabs + distance(i), slabs)
        pair_ref[slab, 0] = dot(ds, q).astype(BF)
        pair_ref[slab, 1] = dot(p.astype(BF), g).astype(BF)
        dq_t = dq_t + dot(k_ref[...].T, ds)
    qb_ref[...] = normalize_back(dq_t.T, q_unit, q_inv).astype(BF)


def attend(me, q, g, pieces):
    rows, width = q.shape
    sizes = [v.shape[0] for v in pieces]
    total = sum(sizes) // 2
    shape = (total // rows, 2, rows, width)
    row_spec = pl.BlockSpec((rows, HD), lambda h, me: (0, h))
    specs = [pl.BlockSpec((n, HD), lambda h, me: (0, h)) for n in sizes]
    return pl.pallas_call(
        attend_body,
        grid_spec=pltpu.PrefetchScalarGridSpec(
            num_scalar_prefetch=1,
            grid=(width // HD,),
            in_specs=[row_spec, row_spec] + specs,
            out_specs=[
                row_spec,
                row_spec,
                pl.BlockSpec((*shape[:3], HD), lambda h, me: (0, 0, 0, h)),
            ],
            scratch_shapes=[pltpu.VMEM((total, rows), F32)],
        ),
        out_shape=[
            jax.ShapeDtypeStruct((rows, width), BF),
            jax.ShapeDtypeStruct((rows, width), BF),
            jax.ShapeDtypeStruct(shape, BF),
        ],
        compiler_params=ARBITRARY,
        name="attend",
    )(me, q, g, *pieces)


def terms_of(x_ref, c_ref, a_ref, b_ref, store):
    slabs, _, own, rows = x_ref.shape
    width = a_ref.shape[1]

    def step(k, carry):
        spots = [2 * k + i for i in range(2)]
        for left_ref, right_ref, cols in (
            (x_ref, a_ref, slice(None, width)),
            (c_ref, b_ref, slice(width, None)),
        ):
            left = jnp.concatenate([left_ref[spot].reshape(2 * own, rows) for spot in spots], axis=0)
            value = dot(left, right_ref[...])
            for i in range(2):
                for y in range(2):
                    at = (2 * i + y) * own
                    store(2 * k + i, y, cols, value[at : at + own])
        return carry

    lax.fori_loop(0, slabs // 2, step, 0)


def query_send_body(x_ref, c_ref, a_ref, b_ref, out_ref):
    def store(r, y, cols, value):
        out_ref[y, r, :, cols] = value.astype(BF)

    terms_of(x_ref, c_ref, a_ref, b_ref, store)


def query_keep_body(x_ref, c_ref, a_ref, b_ref, got_ref, stay_ref, go_ref):
    def store(r, y, cols, value):
        (stay_ref, go_ref)[y][r, :, cols] = (value + got_ref[y, r, :, cols].astype(F32)).astype(BF)

    terms_of(x_ref, c_ref, a_ref, b_ref, store)


def key_send_body(x_ref, k_ref, sum_ref, kb_ref, vb_ref, out_ref):
    width = k_ref.shape[1]
    rows = k_ref.shape[0]
    for h in range(width // HD):
        cols = slice(h * HD, (h + 1) * HD)
        unit, inv = normalize(k_ref[:, cols])
        kb_ref[:, cols] = normalize_back(sum_ref[:rows, cols].astype(F32), unit, inv).astype(BF)
    vb_ref[...] = sum_ref[rows:]

    def store(r, y, cols, value):
        out_ref[r, y, :, cols] = value.astype(BF)

    terms_of(x_ref, x_ref, kb_ref, vb_ref, store)


def key_keep_body(x_ref, a_ref, b_ref, got_ref, stay_ref, y_ref, out_ref):
    own = x_ref.shape[2]

    def store(r, y, cols, value):
        total = value + got_ref[r, y, :, cols].astype(F32)
        out_ref[r, (1 + y) * own : (2 + y) * own, cols] = total.astype(BF)

    terms_of(x_ref, x_ref, a_ref, b_ref, store)
    for r in range(x_ref.shape[0]):
        out_ref[r, :own] = (stay_ref[r].astype(F32) + y_ref[r].astype(F32)).astype(BF)


def call(body, shapes, *operands):
    return pl.pallas_call(
        body,
        in_specs=[VMEM] * len(operands),
        out_shape=[jax.ShapeDtypeStruct(v, BF) for v in shapes],
    )(*operands)


def inner_body(
    me_ref, qb_ref, kb_ref, vb_ref, near_ref, near_far_ref, far_ref, far_far_ref,
    *refs, close,
):
    step = pl.program_id(0)
    qo_refs, (unit_ref, out_ref, sum_ref, both_ref, w_ref) = refs[:4], refs[4:]
    own = qo_refs[0].shape[1]
    width = qb_ref.shape[1]
    away_y, away_c = me_ref[2], me_ref[1]

    def place(refs):
        for c, ref in enumerate(refs):
            for y in range(2):
                spot = lax.rem(away_y + y, 2), lax.rem(away_c + c, 2)
                w_ref[spot[0], spot[1], :, :width] = qo_refs[2 * c + y][0, :, :width]
                w_ref[spot[0], spot[1], :, width:] = ref[0, y * own : (y + 1) * own]

    @pl.when(step < close)
    def _():
        place((near_ref, near_far_ref))

    @pl.when(step >= close)
    def _():
        place((far_ref, far_far_ref))

    low = jnp.concatenate([qb_ref[...], kb_ref[...], vb_ref[...]], axis=1)
    result = dot(low, w_ref[...].reshape(4 * own, 3 * width), 1, 1)
    out_ref[0] = result.astype(BF)
    both = result * unit_ref[...]
    lanes = range(0, result.shape[1], HD)
    plain = sum(result[:, i : i + HD] for i in lanes)
    times = sum(both[:, i : i + HD] for i in lanes)

    @pl.when(step == 0)
    def _():
        sum_ref[...] = plain
        both_ref[...] = times

    @pl.when(step > 0)
    def _():
        sum_ref[...] += plain
        both_ref[...] += times


def inner(me, qb, kb, vb, near, near_far, far, far_far, pieces, unit):
    rows, width = qb.shape
    _, own, both = pieces[0].shape
    close = near.shape[0]
    slabs = close + far.shape[0]

    def place(i, me):
        sign = 1 - 2 * lax.rem(i, 2)
        return lax.rem(me[0] + slabs + lax.div(i + 1, 2) * sign, slabs)

    whole = pl.BlockSpec((rows, width), lambda i, me: (0, 0))
    stat = pl.BlockSpec((rows, HD), lambda i, me: (0, 0))

    def first(rows):
        return pl.BlockSpec((1, rows, both), lambda i, me: (jnp.minimum(i, close - 1), 0, 0))

    def last(rows):
        return pl.BlockSpec((1, rows, both), lambda i, me: (jnp.maximum(i - close, 0), 0, 0))

    return pl.pallas_call(
        lambda *refs: inner_body(*refs, close=close),
        grid_spec=pltpu.PrefetchScalarGridSpec(
            num_scalar_prefetch=1,
            grid=(slabs,),
            in_specs=[whole] * 3
            + [first(2 * own)] * 2
            + [last(2 * own)] * 2
            + [pl.BlockSpec((1, own, both), lambda i, me: (place(i, me), 0, 0))] * 4
            + [pl.BlockSpec((rows, 4 * own), lambda i, me: (0, place(i, me)))],
            out_specs=[
                pl.BlockSpec((1, rows, 4 * own), lambda i, me: (place(i, me), 0, 0)),
                stat,
                stat,
            ],
            scratch_shapes=[pltpu.VMEM((2, 2, own, 3 * width), BF)],
        ),
        out_shape=[
            jax.ShapeDtypeStruct((slabs, rows, 4 * own), BF),
            jax.ShapeDtypeStruct((rows, HD), F32),
            jax.ShapeDtypeStruct((rows, HD), F32),
        ],
        compiler_params=ARBITRARY,
        name="inner",
    )(me, qb, kb, vb, near, near_far, far, far_far, *pieces, unit)


def swap(value, axis):
    return lax.ppermute(value, axis, [(0, 1), (1, 0)])


def turns():
    size = lax.axis_size("seq")
    return [(i, (i + 1) % size) for i in range(size)], [(i, (i - 1) % size) for i in range(size)]


def ring_gather(value, held=None):
    up, down = turns()
    half = value.shape[0] // 2
    rows = [value]
    high = low = value
    for step in range(len(up) // 2 - 1):
        high = lax.ppermute(high, "seq", up)
        low = lax.ppermute(low, "seq", down)
        if step == 0 and held is not None:
            high, low, held = lax.optimization_barrier((high, low, held))
        rows += [high, low]
    rows.append(lax.ppermute(high[:half], "seq", up))
    rows.append(lax.ppermute(low[half:], "seq", down))
    return rows if held is None else (rows, held)


def whole(ring):
    return ring[:-2] + [jnp.concatenate(ring[-2:], axis=0)]


def pieces_of(value):
    parts = []
    for _ in range(3):
        part = lax.reduce_precision(value, 8, 7)
        parts.append(part.astype(BF))
        value = value - part
    return parts


def layer(tokens, cotangent, qkv_weight, out_weight):
    row_count, feature_count = tokens.shape[1:]
    own, _, width = qkv_weight.shape
    slabs = lax.axis_size("seq")
    shares = lax.axis_size(("x", "yhi"))
    me = jnp.stack([lax.axis_index("seq"), lax.axis_index("core"), lax.axis_index("ylo")]).astype(jnp.int32)
    kv_weight = qkv_weight[:, 1:].reshape(own, 2 * width)
    qo_weight = jnp.concatenate([qkv_weight[:, 0], out_weight], axis=1)
    qo_mine = lax.all_gather(qo_weight, "seq")
    kv_y = swap(kv_weight, "ylo")
    kv_weight = jnp.concatenate([kv_weight, kv_y], axis=0)
    unit, inverse, x_keep, x_send, x_r = prepare(me, tokens[0], slabs, True)
    c_keep, c_send, c_r = prepare(me, cotangent[0], slabs, False)
    kv_weight, x_r = lax.optimization_barrier((kv_weight, x_r))
    ring, c_r = ring_gather(kv_weight, c_r)
    ring = whole(ring)
    near, far = jnp.stack(ring[:5]), jnp.stack(ring[5:])
    near_far, far_far = swap(near, "core"), swap(far, "core")
    qo_y = swap(qo_mine, "ylo")
    key, key_value = project_kv(me, x_r, near, near_far, far, far_far)
    every = ring_gather(key_value)
    qo_pieces = (qo_mine, qo_y, swap(qo_mine, "core"), swap(qo_y, "core"))
    query, grad_rows = project_qo(x_r, c_r, *qo_pieces)
    attended, query_back, pair = attend(me, query, grad_rows, every)
    pair = lax.psum_scatter(
        pair.reshape(slabs * 2 * row_count, width), "seq", scatter_dimension=0, tiled=True
    )
    both = 2 * width
    got = swap(call(query_send_body, [(2, slabs, own, both)], x_send, c_send, query_back, attended)[0], "core")
    stay, go = call(query_keep_body, [(slabs, own, both)] * 2, x_keep, c_keep, query_back, attended, got)
    from_y = swap(go, "ylo")
    key, from_y = lax.optimization_barrier((key, from_y))
    key_grad, value_grad, send = call(
        key_send_body, [(row_count, width)] * 2 + [(slabs, 2, own, both)], x_send, key, pair
    )
    merged = call(
        key_keep_body,
        [(slabs, 3 * own, both)],
        x_keep, key_grad, value_grad, swap(send, "core"), stay, from_y,
    )[0]
    merged, key_grad = lax.optimization_barrier((merged, key_grad))
    merged = lax.psum_scatter(
        merged.reshape(slabs * 3 * own, both), "seq", scatter_dimension=0, tiled=True
    )
    query_out = merged[:own].astype(F32)
    key_value_grad = merged[own : 2 * own].astype(F32) + swap(merged[2 * own :], "ylo").astype(F32)
    share, plain, both = inner(
        me, query_back, key_grad, value_grad, near, near_far, far, far_far, qo_pieces, unit
    )
    stats = jnp.stack(pieces_of(jnp.sum(plain, axis=1)) + pieces_of(jnp.sum(both, axis=1)))
    stats = stats.reshape(-1, share.shape[2])
    stats = jnp.pad(stats, ((0, 16 - stats.shape[0]), (0, 0)))
    load = jnp.concatenate([share, jnp.broadcast_to(stats, (shares, *stats.shape))], axis=1)
    load = lax.all_to_all(load, ("x", "yhi"), 0, 0, tiled=True)
    load = load.astype(F32)
    load = jnp.sum(load, axis=0)
    own_share = load[:row_count]
    totals = load[row_count:].reshape(-1)[: 6 * row_count].reshape(2, 3, row_count)
    totals = jnp.sum(totals, axis=1)[:, :, None] / feature_count
    offset = lax.axis_index(("x", "yhi")) * share.shape[2]
    unit_own = lax.dynamic_slice_in_dim(unit, offset, share.shape[2], 1)
    branch = (own_share - totals[0] - unit_own * totals[1]) * inverse[:, :1]
    qkv_grad = jnp.stack(
        [query_out[:, :width], key_value_grad[:, :width], key_value_grad[:, width:]], axis=1
    )
    return (qkv_grad, query_out[:, width:], branch.astype(BF)[None])


def solution(mesh):
    split = jax.sharding.Mesh(
        mesh.devices.reshape(mesh.shape["seq"], mesh.shape["tensor"] // 2, 2, 2, 2),
        ("seq", "x", "yhi", "ylo", "core"),
    )
    blocks = ("seq", "ylo", "core")
    heads = ("x", "yhi")
    return jax.shard_map(
        layer,
        mesh=split,
        in_specs=(
            P(("ylo", "core"), "seq", None),
            P(("ylo", "core"), "seq", None),
            P(blocks, None, heads),
            P(blocks, heads),
        ),
        out_specs=(
            P(blocks, None, heads),
            P(blocks, heads),
            P(("ylo", "core"), "seq", heads),
        ),
        check_vma=False,
    )
```

```python
import jax
import jax.numpy as jnp
from jax import lax
from jax.experimental import pallas as pl
from jax.experimental.pallas import tpu as pltpu
from jax.sharding import PartitionSpec as P

HD = 128
epsilon = 1e-06
BF = jnp.bfloat16
F32 = jnp.float32


def dot(a, b, ca=1, cb=0):
    return lax.dot_general(a, b, (((ca,), (cb,)), ((), ())), preferred_element_type=F32)


def normalize(values, axis=-1):
    average = jnp.mean(values, axis=axis, keepdims=True)
    centered = values - average
    inverse = lax.rsqrt(jnp.mean(centered * centered, axis=axis, keepdims=True) + epsilon)
    return (centered * inverse, inverse)


def normalize_back(gradient, normed, inverse, axis=-1):
    mean_grad = jnp.mean(gradient, axis=axis, keepdims=True)
    mean_both = jnp.mean(gradient * normed, axis=axis, keepdims=True)
    return (gradient - mean_grad - normed * mean_both) * inverse


ARBITRARY = pltpu.CompilerParams(dimension_semantics=("arbitrary",))


def prepare_body(
    me_ref, tok_ref, cot_ref, unit_ref, inv_ref, xk_ref, xs_ref, xr_ref, ck_ref, cs_ref, cr_ref, mean_ref
):
    step = pl.program_id(0)
    rows = tok_ref.shape[0]
    group, _, own, _ = xk_ref.shape
    block = 4 * own
    core = me_ref[1]

    @pl.when(step == 0)
    def _():
        values = tok_ref[...].astype(F32)
        average = jnp.mean(values, axis=-1, keepdims=True)
        centered = values - average
        inverse = lax.rsqrt(jnp.mean(centered * centered, axis=-1, keepdims=True) + epsilon)
        mean_ref[...] = jnp.broadcast_to(average, (rows, HD))
        inv_ref[...] = jnp.broadcast_to(inverse, (rows, HD))

    def slab(s, carry):
        here = pl.ds(pl.multiple_of((step * group + s) * block, HD), block)
        there = pl.ds(pl.multiple_of(s * block, HD), block)
        unit = (tok_ref[:, here].astype(F32) - mean_ref[:, :1]) * inv_ref[:, :1]
        unit_ref[:, there] = unit
        for value, refs in (
            (unit.astype(BF), (xk_ref, xs_ref, xr_ref)),
            (cot_ref[:, here], (ck_ref, cs_ref, cr_ref)),
        ):
            turned = value.T

            def place(refs, turned, c):
                for y in range(2):
                    away_y = lax.rem(me_ref[2] + y, 2)
                    at = (2 * y + c) * own
                    refs[0][s, away_y] = turned[at : at + own]
                    at = (2 * y + 1 - c) * own
                    refs[1][s, away_y] = turned[at : at + own]

            @pl.when(core == 0)
            def _():
                place(refs, turned, 0)

            @pl.when(core == 1)
            def _():
                place(refs, turned, 1)

            for c in range(2):
                refs[2][s, c] = refs[c][s].reshape(2 * own, rows).T
        return carry

    lax.fori_loop(0, group, slab, 0)


def prepare(me, tokens, cotangent, slabs, steps=4):
    rows, features = tokens.shape
    own = features // slabs // 4
    group = slabs // steps
    whole = pl.BlockSpec((rows, features), lambda i, me: (0, 0))
    turned = pl.BlockSpec((group, 2, own, rows), lambda i, me: (i, 0, 0, 0))
    plain = pl.BlockSpec((group, 2, rows, 2 * own), lambda i, me: (i, 0, 0, 0))
    turned_shape = jax.ShapeDtypeStruct((slabs, 2, own, rows), BF)
    plain_shape = jax.ShapeDtypeStruct((slabs, 2, rows, 2 * own), BF)
    return pl.pallas_call(
        prepare_body,
        grid_spec=pltpu.PrefetchScalarGridSpec(
            num_scalar_prefetch=1,
            grid=(steps,),
            in_specs=[whole, whole],
            out_specs=[
                pl.BlockSpec((rows, features // steps), lambda i, me: (0, i)),
                pl.BlockSpec((rows, HD), lambda i, me: (0, 0)),
            ]
            + [turned, turned, plain] * 2,
            scratch_shapes=[pltpu.VMEM((rows, HD), F32)],
        ),
        out_shape=[
            jax.ShapeDtypeStruct((rows, features), F32),
            jax.ShapeDtypeStruct((rows, HD), F32),
        ]
        + [turned_shape, turned_shape, plain_shape] * 2,
        compiler_params=ARBITRARY,
        name="prepare",
    )(me, tokens, cotangent)


def distance(i):
    return (i + 1) // 2 * (1 if i % 2 == 0 else -1)


def project_kv_body(me_ref, x_ref, near_ref, near_far_ref, far_ref, far_far_ref, k_ref, kl_ref, vl_ref):
    slabs = x_ref.shape[0]
    rows, width = k_ref.shape
    close = near_ref.shape[0]
    for n in range(2 * width // 256):
        cols = slice(n * 256, (n + 1) * 256)
        acc = jnp.zeros((rows, 256), F32)
        for i in range(slabs):
            slab = lax.rem(me_ref[0] + slabs + distance(i), slabs)
            if i < close:
                pieces = near_ref[i, :, cols], near_far_ref[i, :, cols]
            else:
                pieces = far_ref[i - close, :, cols], far_far_ref[i - close, :, cols]
            for c, piece in enumerate(pieces):
                acc = acc + dot(x_ref[slab, c], piece)
        for j in range(2):
            at = n * 256 + j * HD
            part = acc[:, j * HD : (j + 1) * HD]
            if at < width:
                k_ref[:, at : at + HD] = part
                kl_ref[:, at : at + HD] = normalize(part)[0].astype(BF)
            else:
                vl_ref[:, at - width : at - width + HD] = part.astype(BF)


def project_kv(me, x, near, near_far, far, far_far):
    rows, width = x.shape[2], near.shape[2] // 2
    return pl.pallas_call(
        project_kv_body,
        in_specs=[pl.BlockSpec(memory_space=pltpu.SMEM)] + [pl.BlockSpec(memory_space=pltpu.VMEM)] * 5,
        out_shape=[
            jax.ShapeDtypeStruct((rows, width), F32),
            jax.ShapeDtypeStruct((rows, width), BF),
            jax.ShapeDtypeStruct((rows, width), BF),
        ],
        name="project_kv",
    )(me, x, near, near_far, far, far_far)


def project_qo_body(x_ref, c_ref, b_ref, by_ref, bc_ref, byc_ref, q_ref, g_ref):
    slabs = x_ref.shape[0]
    rows, width = q_ref.shape
    for left_ref, out_ref, first in ((x_ref, q_ref, 0), (c_ref, g_ref, width)):
        for at, size in ((0, 256), (256, 128)):
            cols = slice(first + at, first + at + size)
            acc = jnp.zeros((rows, size), F32)
            for k in range(slabs):
                for c, (one, two) in enumerate(((b_ref, by_ref), (bc_ref, byc_ref))):
                    piece = jnp.concatenate([one[k, :, cols], two[k, :, cols]], axis=0)
                    acc = acc + dot(left_ref[k, c], piece)
            out_ref[:, at : at + size] = acc.astype(out_ref.dtype)


VMEM = pl.BlockSpec(memory_space=pltpu.VMEM)
SMEM = pl.BlockSpec(memory_space=pltpu.SMEM)


def project_qo(x, c, *pieces):
    rows, width = x.shape[2], pieces[0].shape[2] // 2
    return pl.pallas_call(
        project_qo_body,
        in_specs=[VMEM] * 6,
        out_shape=[jax.ShapeDtypeStruct((rows, width), F32), jax.ShapeDtypeStruct((rows, width), BF)],
        name="project_qo",
    )(x, c, *pieces)


def attend_body(me_ref, q_ref, g_ref, *refs, count):
    k_refs, v_refs = refs[:count], refs[count : 2 * count]
    att_ref, qb_ref, pair_ref, e_ref = refs[2 * count :]
    slabs = pair_ref.shape[0]
    rows = q_ref.shape[0]
    scale = HD ** (-0.5)
    q_unit, q_inv = normalize(q_ref[...])
    q = q_unit.astype(BF)
    g = g_ref[...]
    total = jnp.zeros((8, rows), F32)
    att_t = jnp.zeros((HD, rows), F32)
    at = 0
    spots = []
    for k_ref, v_ref in zip(k_refs, v_refs):
        keys = k_ref.shape[0]
        here = slice(at, at + keys)
        spots.append(here)
        at += keys
        e = jnp.exp(dot(k_ref[...], q, 1, 1) * scale)
        e_ref[here] = e
        total = total + jnp.sum(e.reshape(keys // 8, 8, rows), axis=0)
        att_t = att_t + dot(v_ref[...].T, e.astype(BF))
    total = jnp.sum(total, axis=0, keepdims=True)
    inv_total = 1.0 / total
    att = (att_t * inv_total).T.astype(BF)
    att_ref[...] = att
    delta = jnp.sum((g.astype(F32) * att.astype(F32)).T, axis=0, keepdims=True)
    dq_t = jnp.zeros((HD, rows), F32)
    for i, (k_ref, v_ref, here) in enumerate(zip(k_refs, v_refs, spots)):
        p = e_ref[here] * inv_total
        dp = dot(v_ref[...], g, 1, 1)
        ds = (p * ((dp - delta) * scale)).astype(BF)
        slab = lax.rem(me_ref[0] + slabs + distance(i), slabs)
        pair_ref[slab, 0] = dot(ds, q).astype(BF)
        pair_ref[slab, 1] = dot(p.astype(BF), g).astype(BF)
        dq_t = dq_t + dot(k_ref[...].T, ds)
    qb_ref[...] = normalize_back(dq_t.T, q_unit, q_inv).astype(BF)


def attend(me, q, g, keys, values):
    rows, width = q.shape
    sizes = [k.shape[0] for k in keys]
    shape = (sum(sizes) // rows, 2, rows, width)
    row_spec = pl.BlockSpec((rows, HD), lambda h, me: (0, h))
    specs = [pl.BlockSpec((n, HD), lambda h, me: (0, h)) for n in sizes]
    return pl.pallas_call(
        lambda *refs: attend_body(*refs, count=len(sizes)),
        grid_spec=pltpu.PrefetchScalarGridSpec(
            num_scalar_prefetch=1,
            grid=(width // HD,),
            in_specs=[row_spec, row_spec] + specs * 2,
            out_specs=[
                row_spec,
                row_spec,
                pl.BlockSpec((*shape[:3], HD), lambda h, me: (0, 0, 0, h)),
            ],
            scratch_shapes=[pltpu.VMEM((sum(sizes), rows), F32)],
        ),
        out_shape=[
            jax.ShapeDtypeStruct((rows, width), BF),
            jax.ShapeDtypeStruct((rows, width), BF),
            jax.ShapeDtypeStruct(shape, BF),
        ],
        compiler_params=ARBITRARY,
        name="attend",
    )(me, q, g, *keys, *values)


def terms_of(x_ref, c_ref, a_ref, b_ref, store):
    slabs, _, own, rows = x_ref.shape
    width = a_ref.shape[1]

    def step(k, carry):
        spots = [2 * k + i for i in range(2)]
        for left_ref, right_ref, cols in (
            (x_ref, a_ref, slice(None, width)),
            (c_ref, b_ref, slice(width, None)),
        ):
            left = jnp.concatenate([left_ref[spot].reshape(2 * own, rows) for spot in spots], axis=0)
            value = dot(left, right_ref[...])
            for i in range(2):
                for y in range(2):
                    at = (2 * i + y) * own
                    store(2 * k + i, y, cols, value[at : at + own])
        return carry

    lax.fori_loop(0, slabs // 2, step, 0)


def query_send_body(x_ref, c_ref, a_ref, b_ref, out_ref):
    def store(r, y, cols, value):
        out_ref[y, r, :, cols] = value.astype(BF)

    terms_of(x_ref, c_ref, a_ref, b_ref, store)


def query_keep_body(x_ref, c_ref, a_ref, b_ref, got_ref, stay_ref, go_ref):
    def store(r, y, cols, value):
        (stay_ref, go_ref)[y][r, :, cols] = (value + got_ref[y, r, :, cols].astype(F32)).astype(BF)

    terms_of(x_ref, c_ref, a_ref, b_ref, store)


def key_send_body(x_ref, k_ref, sum_ref, kb_ref, vb_ref, out_ref):
    width = k_ref.shape[1]
    rows = k_ref.shape[0]
    for h in range(width // HD):
        cols = slice(h * HD, (h + 1) * HD)
        unit, inv = normalize(k_ref[:, cols])
        kb_ref[:, cols] = normalize_back(sum_ref[:rows, cols].astype(F32), unit, inv).astype(BF)
    vb_ref[...] = sum_ref[rows:]

    def store(r, y, cols, value):
        out_ref[r, y, :, cols] = value.astype(BF)

    terms_of(x_ref, x_ref, kb_ref, vb_ref, store)


def key_mine_body(x_ref, a_ref, b_ref, stay_ref, y_ref, part_ref, query_ref):
    def store(r, y, cols, value):
        part_ref[r, y, :, cols] = value.astype(BF)

    terms_of(x_ref, x_ref, a_ref, b_ref, store)

    def step(r, carry):
        query_ref[r] = (stay_ref[r].astype(F32) + y_ref[r].astype(F32)).astype(BF)
        return carry

    lax.fori_loop(0, x_ref.shape[0], step, 0)


def key_add_body(part_ref, got_ref, query_ref, out_ref):
    own = part_ref.shape[2]

    def step(r, carry):
        out_ref[r, :own] = query_ref[r]
        for y in range(2):
            total = part_ref[r, y].astype(F32) + got_ref[r, y].astype(F32)
            out_ref[r, (1 + y) * own : (2 + y) * own] = total.astype(BF)
        return carry

    lax.fori_loop(0, part_ref.shape[0], step, 0)


def call(body, shapes, *operands):
    return pl.pallas_call(
        body,
        in_specs=[VMEM] * len(operands),
        out_shape=[jax.ShapeDtypeStruct(v, BF) for v in shapes],
    )(*operands)


def inner_body(
    me_ref, qb_ref, kb_ref, vb_ref, near_ref, near_far_ref, far_ref, far_far_ref,
    *refs, close,
):
    step = pl.program_id(0)
    qo_refs, (unit_ref, out_ref, sum_ref, both_ref, w_ref) = refs[:4], refs[4:]
    own = qo_refs[0].shape[1]
    width = qb_ref.shape[1]
    away_y, away_c = me_ref[2], me_ref[1]

    def place(refs):
        for c, ref in enumerate(refs):
            for y in range(2):
                spot = lax.rem(away_y + y, 2), lax.rem(away_c + c, 2)
                w_ref[spot[0], spot[1], :, :width] = qo_refs[2 * c + y][0, :, :width]
                w_ref[spot[0], spot[1], :, width:] = ref[0, y * own : (y + 1) * own]

    @pl.when(step < close)
    def _():
        place((near_ref, near_far_ref))

    @pl.when(step >= close)
    def _():
        place((far_ref, far_far_ref))

    low = jnp.concatenate([qb_ref[...], kb_ref[...], vb_ref[...]], axis=1)
    result = dot(low, w_ref[...].reshape(4 * own, 3 * width), 1, 1)
    out_ref[0] = result.astype(BF)
    both = result * unit_ref[...]
    lanes = range(0, result.shape[1], HD)
    plain = sum(result[:, i : i + HD] for i in lanes)
    times = sum(both[:, i : i + HD] for i in lanes)

    @pl.when(step == 0)
    def _():
        sum_ref[...] = plain
        both_ref[...] = times

    @pl.when(step > 0)
    def _():
        sum_ref[...] += plain
        both_ref[...] += times


def inner(me, qb, kb, vb, near, near_far, far, far_far, pieces, unit):
    rows, width = qb.shape
    _, own, both = pieces[0].shape
    close = near.shape[0]
    slabs = close + far.shape[0]

    def place(i, me):
        sign = 1 - 2 * lax.rem(i, 2)
        return lax.rem(me[0] + slabs + lax.div(i + 1, 2) * sign, slabs)

    whole = pl.BlockSpec((rows, width), lambda i, me: (0, 0))
    stat = pl.BlockSpec((rows, HD), lambda i, me: (0, 0))

    def first(rows):
        return pl.BlockSpec((1, rows, both), lambda i, me: (jnp.minimum(i, close - 1), 0, 0))

    def last(rows):
        return pl.BlockSpec((1, rows, both), lambda i, me: (jnp.maximum(i - close, 0), 0, 0))

    return pl.pallas_call(
        lambda *refs: inner_body(*refs, close=close),
        grid_spec=pltpu.PrefetchScalarGridSpec(
            num_scalar_prefetch=1,
            grid=(slabs,),
            in_specs=[whole] * 3
            + [first(2 * own)] * 2
            + [last(2 * own)] * 2
            + [pl.BlockSpec((1, own, both), lambda i, me: (place(i, me), 0, 0))] * 4
            + [pl.BlockSpec((rows, 4 * own), lambda i, me: (0, place(i, me)))],
            out_specs=[
                pl.BlockSpec((1, rows, 4 * own), lambda i, me: (place(i, me), 0, 0)),
                stat,
                stat,
            ],
            scratch_shapes=[pltpu.VMEM((2, 2, own, 3 * width), BF)],
        ),
        out_shape=[
            jax.ShapeDtypeStruct((slabs, rows, 4 * own), BF),
            jax.ShapeDtypeStruct((rows, HD), F32),
            jax.ShapeDtypeStruct((rows, HD), F32),
        ],
        compiler_params=ARBITRARY,
        name="inner",
    )(me, qb, kb, vb, near, near_far, far, far_far, *pieces, unit)


def swap(value, axis):
    return lax.ppermute(value, axis, [(0, 1), (1, 0)])


def turns():
    size = lax.axis_size("seq")
    return [(i, (i + 1) % size) for i in range(size)], [(i, (i - 1) % size) for i in range(size)]


def ring_gather(value, held=None, last=None):
    up, down = turns()
    half = value.shape[0] // 2
    rows = [value]
    high = low = value
    for step in range(len(up) // 2 - 1):
        high = lax.ppermute(high, "seq", up)
        low = lax.ppermute(low, "seq", down)
        if step == 0 and held is not None:
            high, low, held = lax.optimization_barrier((high, low, held))
        rows += [high, low]
    if last is None:
        rows.append(lax.ppermute(high[:half], "seq", up))
        rows.append(lax.ppermute(low[half:], "seq", down))
    else:
        rows.append(lax.ppermute(high, "seq", up) if last else lax.ppermute(low, "seq", down))
    return rows if held is None else (rows, held)


def whole(ring):
    return ring[:-2] + [jnp.concatenate(ring[-2:], axis=0)]


def pieces_of(value):
    parts = []
    for _ in range(3):
        part = lax.reduce_precision(value, 8, 7)
        parts.append(part.astype(BF))
        value = value - part
    return parts


def layer(tokens, cotangent, qkv_weight, out_weight):
    row_count, feature_count = tokens.shape[1:]
    own, _, width = qkv_weight.shape
    slabs = lax.axis_size("seq")
    shares = lax.axis_size(("x", "yhi"))
    me = jnp.stack([lax.axis_index("seq"), lax.axis_index("core"), lax.axis_index("ylo")]).astype(jnp.int32)
    kv_weight = qkv_weight[:, 1:].reshape(own, 2 * width)
    qo_weight = jnp.concatenate([qkv_weight[:, 0], out_weight], axis=1)
    qo_mine = lax.all_gather(qo_weight, "seq")
    kv_y = swap(kv_weight, "ylo")
    kv_weight = jnp.concatenate([kv_weight, kv_y], axis=0)
    unit, inverse, *turned = prepare(me, tokens[0], cotangent[0], slabs)
    x_keep, x_send, x_r, c_keep, c_send, c_r = turned
    ring, x_r = ring_gather(kv_weight, x_r)
    ring = whole(ring)
    near, far = jnp.stack(ring[:5]), jnp.stack(ring[5:])
    near_far, far_far = swap(near, "core"), swap(far, "core")
    qo_y = swap(qo_mine, "ylo")
    key, key_low, value_low = project_kv(me, x_r, near, near_far, far, far_far)
    keys = ring_gather(key_low, last=True)
    values = ring_gather(value_low, last=False)
    qo_pieces = (qo_mine, qo_y, swap(qo_mine, "core"), swap(qo_y, "core"))
    query, grad_rows = project_qo(x_r, c_r, *qo_pieces)
    attended, query_back, pair = attend(me, query, grad_rows, keys, values)
    pair = lax.psum_scatter(
        pair.reshape(slabs * 2 * row_count, width), "seq", scatter_dimension=0, tiled=True
    )
    both = 2 * width
    got = swap(call(query_send_body, [(2, slabs, own, both)], x_send, c_send, query_back, attended)[0], "core")
    stay, go = call(query_keep_body, [(slabs, own, both)] * 2, x_keep, c_keep, query_back, attended, got)
    from_y = swap(go, "ylo")
    key, from_y = lax.optimization_barrier((key, from_y))
    key_grad, value_grad, send = call(
        key_send_body, [(row_count, width)] * 2 + [(slabs, 2, own, both)], x_send, key, pair
    )
    got = swap(send, "core")
    part, query_sum = call(
        key_mine_body,
        [(slabs, 2, own, both), (slabs, own, both)],
        x_keep, key_grad, value_grad, stay, from_y,
    )
    merged = call(key_add_body, [(slabs, 3 * own, both)], part, got, query_sum)[0]
    merged, key_grad = lax.optimization_barrier((merged, key_grad))
    merged = lax.psum_scatter(
        merged.reshape(slabs * 3 * own, both), "seq", scatter_dimension=0, tiled=True
    )
    query_out = merged[:own].astype(F32)
    last = swap(merged[2 * own :], "ylo")
    key_value_grad = merged[own : 2 * own].astype(F32) + last.astype(F32)
    share, plain, both = inner(
        me, query_back, key_grad, value_grad, near, near_far, far, far_far, qo_pieces, unit
    )
    stats = jnp.stack(pieces_of(jnp.sum(plain, axis=1)) + pieces_of(jnp.sum(both, axis=1)))
    stats = stats.reshape(-1, share.shape[2])
    stats = jnp.pad(stats, ((0, 16 - stats.shape[0]), (0, 0)))
    load = jnp.concatenate([share, jnp.broadcast_to(stats, (shares, *stats.shape))], axis=1)
    load = lax.all_to_all(load, ("x", "yhi"), 0, 0, tiled=True)
    load = load.astype(F32)
    load = jnp.sum(load, axis=0)
    own_share = load[:row_count]
    totals = load[row_count:].reshape(-1)[: 6 * row_count].reshape(2, 3, row_count)
    totals = jnp.sum(totals, axis=1)[:, :, None] / feature_count
    offset = lax.axis_index(("x", "yhi")) * share.shape[2]
    unit_own = lax.dynamic_slice_in_dim(unit, offset, share.shape[2], 1)
    branch = ((own_share - totals[0] - unit_own * totals[1]) * inverse[:, :1]).astype(BF)
    qkv_grad = jnp.stack(
        [query_out[:, :width], key_value_grad[:, :width], key_value_grad[:, width:]], axis=1
    )
    return (qkv_grad, query_out[:, width:], branch[None])


def solution(mesh):
    split = jax.sharding.Mesh(
        mesh.devices.reshape(mesh.shape["seq"], mesh.shape["tensor"] // 2, 2, 2, 2),
        ("seq", "x", "yhi", "ylo", "core"),
    )
    blocks = ("seq", "ylo", "core")
    heads = ("x", "yhi")
    return jax.shard_map(
        layer,
        mesh=split,
        in_specs=(
            P(("ylo", "core"), "seq", None),
            P(("ylo", "core"), "seq", None),
            P(blocks, None, heads),
            P(blocks, heads),
        ),
        out_specs=(
            P(blocks, None, heads),
            P(blocks, heads),
            P(("ylo", "core"), "seq", heads),
        ),
        check_vma=False,
    )
```

```python
import jax
import jax.numpy as jnp
from jax import lax
from jax.experimental import pallas as pl
from jax.experimental.pallas import tpu as pltpu
from jax.sharding import PartitionSpec as P

HD = 128
epsilon = 1e-06
BF = jnp.bfloat16
F32 = jnp.float32


def dot(a, b, ca=1, cb=0):
    return lax.dot_general(a, b, (((ca,), (cb,)), ((), ())), preferred_element_type=F32)


def normalize(values, axis=-1):
    average = jnp.mean(values, axis=axis, keepdims=True)
    centered = values - average
    inverse = lax.rsqrt(jnp.mean(centered * centered, axis=axis, keepdims=True) + epsilon)
    return (centered * inverse, inverse)


def normalize_back(gradient, normed, inverse, axis=-1):
    mean_grad = jnp.mean(gradient, axis=axis, keepdims=True)
    mean_both = jnp.mean(gradient * normed, axis=axis, keepdims=True)
    return (gradient - mean_grad - normed * mean_both) * inverse


ARBITRARY = pltpu.CompilerParams(dimension_semantics=("arbitrary",))


def prepare_body(
    me_ref, tok_ref, cot_ref, unit_ref, inv_ref, xk_ref, xs_ref, xr_ref, ck_ref, cs_ref, cr_ref, mean_ref
):
    step = pl.program_id(0)
    rows = tok_ref.shape[0]
    group, _, own, _ = xk_ref.shape
    block = 4 * own
    core = me_ref[1]

    @pl.when(step == 0)
    def _():
        values = tok_ref[...].astype(F32)
        average = jnp.mean(values, axis=-1, keepdims=True)
        centered = values - average
        inverse = lax.rsqrt(jnp.mean(centered * centered, axis=-1, keepdims=True) + epsilon)
        mean_ref[...] = jnp.broadcast_to(average, (rows, HD))
        inv_ref[...] = jnp.broadcast_to(inverse, (rows, HD))

    def slab(s, carry):
        here = pl.ds(pl.multiple_of((step * group + s) * block, HD), block)
        there = pl.ds(pl.multiple_of(s * block, HD), block)
        unit = (tok_ref[:, here].astype(F32) - mean_ref[:, :1]) * inv_ref[:, :1]
        unit_ref[:, there] = unit
        for value, refs in (
            (unit.astype(BF), (xk_ref, xs_ref, xr_ref)),
            (cot_ref[:, here], (ck_ref, cs_ref, cr_ref)),
        ):
            turned = value.T

            def place(refs, turned, c):
                for y in range(2):
                    away_y = lax.rem(me_ref[2] + y, 2)
                    at = (2 * y + c) * own
                    refs[0][s, away_y] = turned[at : at + own]
                    at = (2 * y + 1 - c) * own
                    refs[1][s, away_y] = turned[at : at + own]

            @pl.when(core == 0)
            def _():
                place(refs, turned, 0)

            @pl.when(core == 1)
            def _():
                place(refs, turned, 1)

            for c in range(2):
                refs[2][s, c] = refs[c][s].reshape(2 * own, rows).T
        return carry

    lax.fori_loop(0, group, slab, 0)


def prepare(me, tokens, cotangent, slabs, steps=4):
    rows, features = tokens.shape
    own = features // slabs // 4
    group = slabs // steps
    whole = pl.BlockSpec((rows, features), lambda i, me: (0, 0))
    turned = pl.BlockSpec((group, 2, own, rows), lambda i, me: (i, 0, 0, 0))
    plain = pl.BlockSpec((group, 2, rows, 2 * own), lambda i, me: (i, 0, 0, 0))
    turned_shape = jax.ShapeDtypeStruct((slabs, 2, own, rows), BF)
    plain_shape = jax.ShapeDtypeStruct((slabs, 2, rows, 2 * own), BF)
    return pl.pallas_call(
        prepare_body,
        grid_spec=pltpu.PrefetchScalarGridSpec(
            num_scalar_prefetch=1,
            grid=(steps,),
            in_specs=[whole, whole],
            out_specs=[
                pl.BlockSpec((rows, features // steps), lambda i, me: (0, i)),
                pl.BlockSpec((rows, HD), lambda i, me: (0, 0)),
            ]
            + [turned, turned, plain] * 2,
            scratch_shapes=[pltpu.VMEM((rows, HD), F32)],
        ),
        out_shape=[
            jax.ShapeDtypeStruct((rows, features), F32),
            jax.ShapeDtypeStruct((rows, HD), F32),
        ]
        + [turned_shape, turned_shape, plain_shape] * 2,
        compiler_params=ARBITRARY,
        name="prepare",
    )(me, tokens, cotangent)


def distance(i):
    return (i + 1) // 2 * (1 if i % 2 == 0 else -1)


def project_near_body(me_ref, x_ref, mine_ref, theirs_ref, acc_ref):
    slabs = x_ref.shape[0]
    for at in range(0, acc_ref.shape[1], 256):
        cols = slice(at, at + 256)
        acc = jnp.zeros((acc_ref.shape[0], 256), F32)
        for i in range(mine_ref.shape[0]):
            slab = lax.rem(me_ref[0] + slabs + distance(i), slabs)
            acc = acc + dot(x_ref[slab, 0], mine_ref[i, :, cols])
            acc = acc + dot(x_ref[slab, 1], theirs_ref[i, :, cols])
        acc_ref[:, cols] = acc


def project_far_body(me_ref, x_ref, near_ref, mine_ref, theirs_ref, k_ref, kl_ref, vl_ref):
    slabs = x_ref.shape[0]
    width = k_ref.shape[1]
    close = slabs - mine_ref.shape[0]
    for first in range(0, 2 * width, 256):
        cols = slice(first, first + 256)
        acc = near_ref[:, cols]
        for i in range(mine_ref.shape[0]):
            slab = lax.rem(me_ref[0] + slabs + distance(close + i), slabs)
            acc = acc + dot(x_ref[slab, 0], mine_ref[i, :, cols])
            acc = acc + dot(x_ref[slab, 1], theirs_ref[i, :, cols])
        for at in range(first, first + 256, HD):
            part = acc[:, at - first : at - first + HD]
            if at < width:
                k_ref[:, at : at + HD] = part
                kl_ref[:, at : at + HD] = normalize(part)[0].astype(BF)
            else:
                vl_ref[:, at - width : at - width + HD] = part.astype(BF)


def project_near(me, x, mine, theirs):
    return pl.pallas_call(
        project_near_body,
        in_specs=[SMEM] + [VMEM] * 3,
        out_shape=jax.ShapeDtypeStruct((x.shape[2], mine.shape[2]), F32),
        name="project_near",
    )(me, x, mine, theirs)


def project_far(me, x, acc, mine, theirs):
    shape = (acc.shape[0], acc.shape[1] // 2)
    return pl.pallas_call(
        project_far_body,
        in_specs=[SMEM] + [VMEM] * 4,
        out_shape=[
            jax.ShapeDtypeStruct(shape, F32),
            jax.ShapeDtypeStruct(shape, BF),
            jax.ShapeDtypeStruct(shape, BF),
        ],
        name="project_far",
    )(me, x, acc, mine, theirs)


def project_qo_body(x_ref, c_ref, b_ref, by_ref, bc_ref, byc_ref, q_ref, g_ref):
    slabs = x_ref.shape[0]
    rows, width = q_ref.shape
    for left_ref, out_ref, first in ((x_ref, q_ref, 0), (c_ref, g_ref, width)):
        for at, size in ((0, 256), (256, 128)):
            cols = slice(first + at, first + at + size)
            acc = jnp.zeros((rows, size), F32)
            for k in range(slabs):
                for c, (one, two) in enumerate(((b_ref, by_ref), (bc_ref, byc_ref))):
                    piece = jnp.concatenate([one[k, :, cols], two[k, :, cols]], axis=0)
                    acc = acc + dot(left_ref[k, c], piece)
            out_ref[:, at : at + size] = acc.astype(out_ref.dtype)


VMEM = pl.BlockSpec(memory_space=pltpu.VMEM)
SMEM = pl.BlockSpec(memory_space=pltpu.SMEM)


def project_qo(x, c, *pieces):
    rows, width = x.shape[2], pieces[0].shape[2] // 2
    return pl.pallas_call(
        project_qo_body,
        in_specs=[VMEM] * 6,
        out_shape=[jax.ShapeDtypeStruct((rows, width), F32), jax.ShapeDtypeStruct((rows, width), BF)],
        name="project_qo",
    )(x, c, *pieces)


def attend_body(me_ref, q_ref, g_ref, *refs, count):
    k_refs, v_refs = refs[:count], refs[count : 2 * count]
    att_ref, qb_ref, pair_ref, e_ref = refs[2 * count :]
    slabs = pair_ref.shape[0]
    rows = q_ref.shape[0]
    scale = HD ** (-0.5)
    q_unit, q_inv = normalize(q_ref[...])
    q = q_unit.astype(BF)
    g = g_ref[...]
    total = jnp.zeros((8, rows), F32)
    att_t = jnp.zeros((HD, rows), F32)
    at = 0
    spots = []
    for k_ref, v_ref in zip(k_refs, v_refs):
        keys = k_ref.shape[0]
        here = slice(at, at + keys)
        spots.append(here)
        at += keys
        e = jnp.exp(dot(k_ref[...], q, 1, 1) * scale)
        e_ref[here] = e
        total = total + jnp.sum(e.reshape(keys // 8, 8, rows), axis=0)
        att_t = att_t + dot(v_ref[...].T, e.astype(BF))
    total = jnp.sum(total, axis=0, keepdims=True)
    inv_total = 1.0 / total
    att = (att_t * inv_total).T.astype(BF)
    att_ref[...] = att
    delta = jnp.sum((g.astype(F32) * att.astype(F32)).T, axis=0, keepdims=True)
    dq_t = jnp.zeros((HD, rows), F32)
    for i, (k_ref, v_ref, here) in enumerate(zip(k_refs, v_refs, spots)):
        p = e_ref[here] * inv_total
        dp = dot(v_ref[...], g, 1, 1)
        ds = (p * ((dp - delta) * scale)).astype(BF)
        slab = lax.rem(me_ref[0] + slabs + distance(i), slabs)
        pair_ref[slab, 0] = dot(ds, q).astype(BF)
        pair_ref[slab, 1] = dot(p.astype(BF), g).astype(BF)
        dq_t = dq_t + dot(k_ref[...].T, ds)
    qb_ref[...] = normalize_back(dq_t.T, q_unit, q_inv).astype(BF)


def attend(me, q, g, keys, values):
    rows, width = q.shape
    sizes = [k.shape[0] for k in keys]
    shape = (sum(sizes) // rows, 2, rows, width)
    row_spec = pl.BlockSpec((rows, HD), lambda h, me: (0, h))
    specs = [pl.BlockSpec((n, HD), lambda h, me: (0, h)) for n in sizes]
    return pl.pallas_call(
        lambda *refs: attend_body(*refs, count=len(sizes)),
        grid_spec=pltpu.PrefetchScalarGridSpec(
            num_scalar_prefetch=1,
            grid=(width // HD,),
            in_specs=[row_spec, row_spec] + specs * 2,
            out_specs=[
                row_spec,
                row_spec,
                pl.BlockSpec((*shape[:3], HD), lambda h, me: (0, 0, 0, h)),
            ],
            scratch_shapes=[pltpu.VMEM((sum(sizes), rows), F32)],
        ),
        out_shape=[
            jax.ShapeDtypeStruct((rows, width), BF),
            jax.ShapeDtypeStruct((rows, width), BF),
            jax.ShapeDtypeStruct(shape, BF),
        ],
        compiler_params=ARBITRARY,
        name="attend",
    )(me, q, g, *keys, *values)


def terms_of(x_ref, c_ref, a_ref, b_ref, store):
    slabs, _, own, rows = x_ref.shape
    width = a_ref.shape[1]

    def step(k, carry):
        spots = [2 * k + i for i in range(2)]
        for left_ref, right_ref, cols in (
            (x_ref, a_ref, slice(None, width)),
            (c_ref, b_ref, slice(width, None)),
        ):
            left = jnp.concatenate([left_ref[spot].reshape(2 * own, rows) for spot in spots], axis=0)
            value = dot(left, right_ref[...])
            for i in range(2):
                for y in range(2):
                    at = (2 * i + y) * own
                    store(2 * k + i, y, cols, value[at : at + own])
        return carry

    lax.fori_loop(0, slabs // 2, step, 0)


def query_send_body(x_ref, c_ref, a_ref, b_ref, out_ref):
    def store(r, y, cols, value):
        out_ref[y, r, :, cols] = value.astype(BF)

    terms_of(x_ref, c_ref, a_ref, b_ref, store)


def query_keep_body(x_ref, c_ref, a_ref, b_ref, got_ref, stay_ref, go_ref):
    def store(r, y, cols, value):
        (stay_ref, go_ref)[y][r, :, cols] = (value + got_ref[y, r, :, cols].astype(F32)).astype(BF)

    terms_of(x_ref, c_ref, a_ref, b_ref, store)


def key_send_body(x_ref, k_ref, sum_ref, kb_ref, vb_ref, out_ref):
    width = k_ref.shape[1]
    rows = k_ref.shape[0]
    for h in range(width // HD):
        cols = slice(h * HD, (h + 1) * HD)
        unit, inv = normalize(k_ref[:, cols])
        kb_ref[:, cols] = normalize_back(sum_ref[:rows, cols].astype(F32), unit, inv).astype(BF)
    vb_ref[...] = sum_ref[rows:]

    def store(r, y, cols, value):
        out_ref[r, y, :, cols] = value.astype(BF)

    terms_of(x_ref, x_ref, kb_ref, vb_ref, store)


def key_mine_body(x_ref, a_ref, b_ref, stay_ref, y_ref, part_ref, query_ref):
    def store(r, y, cols, value):
        part_ref[r, y, :, cols] = value.astype(BF)

    terms_of(x_ref, x_ref, a_ref, b_ref, store)

    def step(r, carry):
        query_ref[r] = (stay_ref[r].astype(F32) + y_ref[r].astype(F32)).astype(BF)
        return carry

    lax.fori_loop(0, x_ref.shape[0], step, 0)


def key_add_body(part_ref, got_ref, query_ref, out_ref, held_ref, sem_ref):
    own = part_ref.shape[2]
    group = part_ref.shape[0]
    step = pl.program_id(0)

    def fetch(i):
        here = pl.ds(i * group, group)
        return pltpu.make_async_copy(got_ref.at[here], held_ref.at[here], sem_ref.at[i])

    @pl.when(step == 0)
    def _():
        for i in range(got_ref.shape[0] // group):
            fetch(i).start()

    fetch(step).wait()
    for r in range(group):
        out_ref[r, :own] = query_ref[r]
        for y in range(2):
            total = part_ref[r, y].astype(F32) + held_ref[step * group + r, y].astype(F32)
            out_ref[r, (1 + y) * own : (2 + y) * own] = total.astype(BF)


def key_add(part, got, query, steps=4):
    slabs, _, own, both = part.shape
    group = slabs // steps
    return pl.pallas_call(
        key_add_body,
        grid=(steps,),
        in_specs=[
            pl.BlockSpec((group, 2, own, both), lambda i: (i, 0, 0, 0)),
            pl.BlockSpec(memory_space=pltpu.HBM),
            pl.BlockSpec((group, own, both), lambda i: (i, 0, 0)),
        ],
        out_specs=pl.BlockSpec((group, 3 * own, both), lambda i: (i, 0, 0)),
        out_shape=jax.ShapeDtypeStruct((slabs, 3 * own, both), BF),
        scratch_shapes=[pltpu.VMEM(part.shape, BF), pltpu.SemaphoreType.DMA((steps,))],
        compiler_params=ARBITRARY,
        name="key_add",
    )(part, got, query)


def call(body, shapes, *operands):
    return pl.pallas_call(
        body,
        in_specs=[VMEM] * len(operands),
        out_shape=[jax.ShapeDtypeStruct(v, BF) for v in shapes],
    )(*operands)


def inner_body(
    me_ref, qb_ref, kb_ref, vb_ref, near_ref, near_far_ref, far_ref, far_far_ref,
    *refs, close,
):
    step = pl.program_id(0)
    qo_refs, (unit_ref, out_ref, sum_ref, both_ref, w_ref) = refs[:4], refs[4:]
    own = qo_refs[0].shape[1]
    width = qb_ref.shape[1]
    away_y, away_c = me_ref[2], me_ref[1]

    def place(refs):
        for c, ref in enumerate(refs):
            for y in range(2):
                spot = lax.rem(away_y + y, 2), lax.rem(away_c + c, 2)
                w_ref[spot[0], spot[1], :, :width] = qo_refs[2 * c + y][0, :, :width]
                w_ref[spot[0], spot[1], :, width:] = ref[0, y * own : (y + 1) * own]

    @pl.when(step < close)
    def _():
        place((near_ref, near_far_ref))

    @pl.when(step >= close)
    def _():
        place((far_ref, far_far_ref))

    low = jnp.concatenate([qb_ref[...], kb_ref[...], vb_ref[...]], axis=1)
    result = dot(low, w_ref[...].reshape(4 * own, 3 * width), 1, 1)
    out_ref[0] = result.astype(BF)
    both = result * unit_ref[...]
    lanes = range(0, result.shape[1], HD)
    plain = sum(result[:, i : i + HD] for i in lanes)
    times = sum(both[:, i : i + HD] for i in lanes)

    @pl.when(step == 0)
    def _():
        sum_ref[...] = plain
        both_ref[...] = times

    @pl.when(step > 0)
    def _():
        sum_ref[...] += plain
        both_ref[...] += times


def inner(me, qb, kb, vb, near, near_far, far, far_far, pieces, unit):
    rows, width = qb.shape
    _, own, both = pieces[0].shape
    close = near.shape[0]
    slabs = close + far.shape[0]

    def place(i, me):
        sign = 1 - 2 * lax.rem(i, 2)
        return lax.rem(me[0] + slabs + lax.div(i + 1, 2) * sign, slabs)

    whole = pl.BlockSpec((rows, width), lambda i, me: (0, 0))
    stat = pl.BlockSpec((rows, HD), lambda i, me: (0, 0))

    def first(rows):
        return pl.BlockSpec((1, rows, both), lambda i, me: (jnp.minimum(i, close - 1), 0, 0))

    def last(rows):
        return pl.BlockSpec((1, rows, both), lambda i, me: (jnp.maximum(i - close, 0), 0, 0))

    return pl.pallas_call(
        lambda *refs: inner_body(*refs, close=close),
        grid_spec=pltpu.PrefetchScalarGridSpec(
            num_scalar_prefetch=1,
            grid=(slabs,),
            in_specs=[whole] * 3
            + [first(2 * own)] * 2
            + [last(2 * own)] * 2
            + [pl.BlockSpec((1, own, both), lambda i, me: (place(i, me), 0, 0))] * 4
            + [pl.BlockSpec((rows, 4 * own), lambda i, me: (0, place(i, me)))],
            out_specs=[
                pl.BlockSpec((1, rows, 4 * own), lambda i, me: (place(i, me), 0, 0)),
                stat,
                stat,
            ],
            scratch_shapes=[pltpu.VMEM((2, 2, own, 3 * width), BF)],
        ),
        out_shape=[
            jax.ShapeDtypeStruct((slabs, rows, 4 * own), BF),
            jax.ShapeDtypeStruct((rows, HD), F32),
            jax.ShapeDtypeStruct((rows, HD), F32),
        ],
        compiler_params=ARBITRARY,
        name="inner",
    )(me, qb, kb, vb, near, near_far, far, far_far, *pieces, unit)


def swap(value, axis):
    return lax.ppermute(value, axis, [(0, 1), (1, 0)])


def turns():
    size = lax.axis_size("seq")
    return [(i, (i + 1) % size) for i in range(size)], [(i, (i - 1) % size) for i in range(size)]


def ring_gather(value, held=None, last=None):
    up, down = turns()
    half = value.shape[0] // 2
    rows = [value]
    high = low = value
    for step in range(len(up) // 2 - 1):
        high = lax.ppermute(high, "seq", up)
        low = lax.ppermute(low, "seq", down)
        if step == 0 and held is not None:
            high, low, held = lax.optimization_barrier((high, low, held))
        rows += [high, low]
    if last is None:
        rows.append(lax.ppermute(high[:half], "seq", up))
        rows.append(lax.ppermute(low[half:], "seq", down))
    else:
        rows.append(lax.ppermute(high, "seq", up) if last else lax.ppermute(low, "seq", down))
    return rows if held is None else (rows, held)


def whole(ring):
    return ring[:-2] + [jnp.concatenate(ring[-2:], axis=0)]


def pieces_of(value):
    parts = []
    for _ in range(3):
        part = lax.reduce_precision(value, 8, 7)
        parts.append(part.astype(BF))
        value = value - part
    return parts


def layer(tokens, cotangent, qkv_weight, out_weight):
    row_count, feature_count = tokens.shape[1:]
    own, _, width = qkv_weight.shape
    slabs = lax.axis_size("seq")
    shares = lax.axis_size(("x", "yhi"))
    me = jnp.stack([lax.axis_index("seq"), lax.axis_index("core"), lax.axis_index("ylo")]).astype(jnp.int32)
    kv_weight = qkv_weight[:, 1:].reshape(own, 2 * width)
    qo_weight = jnp.concatenate([qkv_weight[:, 0], out_weight], axis=1)
    qo_mine = lax.all_gather(qo_weight, "seq")
    kv_y = swap(kv_weight, "ylo")
    kv_weight = jnp.concatenate([kv_weight, kv_y], axis=0)
    unit, inverse, *turned = prepare(me, tokens[0], cotangent[0], slabs)
    x_keep, x_send, x_r, c_keep, c_send, c_r = turned
    ring, x_r = ring_gather(kv_weight, x_r)
    ring = whole(ring)
    near, far = jnp.stack(ring[:5]), jnp.stack(ring[5:])
    near_far = swap(near, "core")
    far_far = swap(far, "core")
    acc = project_near(me, x_r, near, near_far)
    qo_y = swap(qo_mine, "ylo")
    key, key_low, value_low = project_far(me, x_r, acc, far, far_far)
    keys = ring_gather(key_low, last=True)
    values = ring_gather(value_low, last=False)
    qo_pieces = (qo_mine, qo_y, swap(qo_mine, "core"), swap(qo_y, "core"))
    query, grad_rows = project_qo(x_r, c_r, *qo_pieces)
    attended, query_back, pair = attend(me, query, grad_rows, keys, values)
    pair = lax.psum_scatter(
        pair.reshape(slabs * 2 * row_count, width), "seq", scatter_dimension=0, tiled=True
    )
    both = 2 * width
    got = swap(call(query_send_body, [(2, slabs, own, both)], x_send, c_send, query_back, attended)[0], "core")
    stay, go = call(query_keep_body, [(slabs, own, both)] * 2, x_keep, c_keep, query_back, attended, got)
    from_y = swap(go, "ylo")
    key, from_y = lax.optimization_barrier((key, from_y))
    key_grad, value_grad, send = call(
        key_send_body, [(row_count, width)] * 2 + [(slabs, 2, own, both)], x_send, key, pair
    )
    got = swap(send, "core")
    part, query_sum = call(
        key_mine_body,
        [(slabs, 2, own, both), (slabs, own, both)],
        x_keep, key_grad, value_grad, stay, from_y,
    )
    merged = key_add(part, got, query_sum)
    merged, key_grad = lax.optimization_barrier((merged, key_grad))
    merged = lax.psum_scatter(
        merged.reshape(slabs * 3 * own, both), "seq", scatter_dimension=0, tiled=True
    )
    query_out = merged[:own].astype(F32)
    last = swap(merged[2 * own :], "ylo")
    key_value_grad = merged[own : 2 * own].astype(F32) + last.astype(F32)
    share, plain, both = inner(
        me, query_back, key_grad, value_grad, near, near_far, far, far_far, qo_pieces, unit
    )
    stats = jnp.stack(pieces_of(jnp.sum(plain, axis=1)) + pieces_of(jnp.sum(both, axis=1)))
    stats = stats.reshape(-1, share.shape[2])
    stats = jnp.pad(stats, ((0, 16 - stats.shape[0]), (0, 0)))
    load = jnp.concatenate([share, jnp.broadcast_to(stats, (shares, *stats.shape))], axis=1)
    load = lax.all_to_all(load, ("x", "yhi"), 0, 0, tiled=True)
    load = load.astype(F32)
    load = jnp.sum(load, axis=0)
    own_share = load[:row_count]
    totals = load[row_count:].reshape(-1)[: 6 * row_count].reshape(2, 3, row_count)
    totals = jnp.sum(totals, axis=1)[:, :, None] / feature_count
    offset = lax.axis_index(("x", "yhi")) * share.shape[2]
    unit_own = lax.dynamic_slice_in_dim(unit, offset, share.shape[2], 1)
    branch = ((own_share - totals[0] - unit_own * totals[1]) * inverse[:, :1]).astype(BF)
    qkv_grad = jnp.stack(
        [query_out[:, :width], key_value_grad[:, :width], key_value_grad[:, width:]], axis=1
    )
    return (qkv_grad, query_out[:, width:], branch[None])


def solution(mesh):
    split = jax.sharding.Mesh(
        mesh.devices.reshape(mesh.shape["seq"], mesh.shape["tensor"] // 2, 2, 2, 2),
        ("seq", "x", "yhi", "ylo", "core"),
    )
    blocks = ("seq", "ylo", "core")
    heads = ("x", "yhi")
    return jax.shard_map(
        layer,
        mesh=split,
        in_specs=(
            P(("ylo", "core"), "seq", None),
            P(("ylo", "core"), "seq", None),
            P(blocks, None, heads),
            P(blocks, heads),
        ),
        out_specs=(
            P(blocks, None, heads),
            P(blocks, heads),
            P(("ylo", "core"), "seq", heads),
        ),
        check_vma=False,
    )
```
